512 devices in a mesh: cuts: 32 (over z, y_lo), slab: 16 (over x, y_hi, core).
Axes of the slice: x: 4, y: 8 (y_hi: 2, y_lo: 4; y = y_hi * 4 + y_lo), z: 8, core: 2. Of those that a mesh axis runs over, the one named last changes fastest.
Arguments:
- quasi: bfloat16 [2, 192, 16, 9216], P(None, 'cuts', 'slab'), may hold values from -6 to 6
- counts: int32 [32], replicated, may hold values from 1 to 6, 64 in all
- slot_slice: int32 [192], replicated, may hold values from 0 to 15
- occupation: float32 [192], replicated, may hold values from 0.0078125 to 0.0625
- filter_coef: float32 [16, 9], replicated, may hold values from -2.5 to 2.5
- trap_index: int32 [16, 9216], P('slab'), may hold values from 0 to 31
- trap_table: float32 [32], replicated, may hold values from 0 to 1.5
- mean_field: float32 [16, 9216], P('slab'), may hold values from -1.5 to 0
- pairing: float32 [16, 9216], P('slab'), may hold values from 0.2 to 1
Outputs:
- normal_density: float32 [16, 9216], P('slab', 'cuts')
- anomalous_density: float32 [16, 9216], P('slab', 'cuts')
- new_mean_field: float32 [16, 9216], P('slab', 'cuts')
- new_pairing: float32 [16, 9216], P('slab', 'cuts')
The draws below stay inside these ranges and needn't reach their ends.
Inputs may be any that keep to these rules, and one draw needn't show every extreme that they name: The live vectors of cut c fill the first counts[c] of its 6 slots; the counts sum to 64 and the largest is exactly 6.
All inputs are finite; a program needn't handle non-finite values.
Results may differ from the reference program's by a relative error of at most 0.0003.
Values may be sent and summed in bfloat16 or wider, within the bound.
No kernel may reach another device: no remote copies, remote signals or barrier semaphores. Data moves between devices by JAX's collectives and lax.ppermute only.
A program may use at most 64 MiB of HBM per device.

```python
import math
import jax
import jax.numpy as jnp
import numpy as np
from jax import lax

NX = 96
NY = 96
DEGREE = 8
SLICES = 16
LEVELS = 32
CAP = 6
SLOTS = 192
VECS = 64
NZ = 16
N_CUTS = 32


def draw_quasi(key, part):
    jitter_part = jax.random.normal(jax.random.fold_in(key, 11), (2, SLOTS, NZ, NY * NX), jnp.float32)
    values = jitter_part
    return jnp.clip(values, -6.0, 6.0).astype(jnp.bfloat16)


def draw_filter_coef(key, part):
    baseline = 0.35 * jax.random.normal(jax.random.fold_in(key, 21), (SLICES, DEGREE + 1), jnp.float32)
    values = baseline
    return jnp.clip(values, -2.5, 2.5).astype(jnp.float32)


def draw_trap_table(key, part):
    values = jax.random.uniform(jax.random.fold_in(key, 31), (LEVELS,), jnp.float32, 0.0, 1.5)
    return values.astype(jnp.float32)


def draw_mean_field(key, part):
    values = jax.random.uniform(jax.random.fold_in(key, 41), (NZ, NY * NX), jnp.float32, -1.5, 0.0)
    return values.astype(jnp.float32)


def touch_ends(entries, rng, smallest, top_value):
    shape = entries.shape
    spot = [jax.random.randint(jax.random.fold_in(rng, axis), (), 0, shape[axis]) for axis in range(len(shape))]
    entries = entries.at[tuple(spot)].set(smallest)
    longest = shape.index(max(shape))
    spot[longest] = (spot[longest] + 1) % shape[longest]
    return entries.at[tuple(spot)].set(top_value)


def shard_levels(key, shape, pieces, smallest, high):
    loudness, own = 1.0, jax.random.fold_in(key, 6)
    for dim, shards_of in pieces:
        steps = jnp.exp(jax.random.uniform(jax.random.fold_in(own, dim), (shards_of,), jnp.float32, smallest / len(pieces), high / len(pieces)))
        loudness = loudness * jnp.repeat(steps, shape[dim] // shards_of).reshape([-1 if axis == dim else 1 for axis in range(len(shape))])
    return loudness


def split_up(number_of, total, bound, lean):
    loads = [(1 << 20) // math.isqrt(grade ** lean) + 1 for grade in range(2, number_of + 1)]
    rest, holding = total - bound - (number_of - 1), [1] * (number_of - 1)
    while rest > 0:
        free = [i for i in range(number_of - 1) if holding[i] < bound]
        pool, remaining = sum([loads[i] for i in free]), rest
        for i in free:
            extra = min(bound - holding[i], max(1, remaining * loads[i] // pool), rest)
            holding[i] = holding[i] + extra
            rest = rest - extra
    return np.array([bound] + holding)


def uneven(key, count, total, limit, slope):
    if count == 2:
        one = jax.random.randint(key, (), max(1, total - limit), min(limit, total - 1) + 1)
        return jnp.stack([one, total - one])
    tallies = jnp.asarray(split_up(count, total, limit, slope), jnp.int32)
    pairs = (count - 1) // 2
    source_of, taker = tallies[1:1 + 2 * pairs:2], tallies[2:2 + 2 * pairs:2]
    room = jnp.minimum(source_of - 1, limit - taker)
    passed = jax.random.randint(jax.random.fold_in(key, 1), (pairs,), 0, 1 << 20) % (room + 1)
    tallies = tallies.at[1:1 + 2 * pairs:2].set(source_of - passed).at[2:2 + 2 * pairs:2].set(taker + passed)
    return tallies[jax.random.permutation(jax.random.fold_in(key, 2), count)]


def setup_inputs(seed: int = 0) -> dict:
    arg_keys = jax.random.split(jax.random.key(seed), 10)
    quasi = draw_quasi(jax.random.fold_in(arg_keys[9], 71), 0)
    counts = uneven(arg_keys[1], N_CUTS, VECS, CAP, 2).astype(jnp.int32)
    slot_slice = touch_ends(jax.random.randint(arg_keys[2], (SLOTS,), 0, SLICES), jax.random.fold_in(arg_keys[2], 1), 0, SLICES - 1).astype(jnp.int32)
    occupation = jnp.clip(jnp.exp(jax.random.uniform(arg_keys[3], (SLOTS,), jnp.float32, math.log(0.0078125), math.log(0.0625))), 0.0078125, 0.0625)
    filter_coef = draw_filter_coef(jax.random.fold_in(arg_keys[9], 71), 0)
    trap_index = touch_ends(jax.random.randint(arg_keys[5], (NZ, NY * NX), 0, LEVELS), jax.random.fold_in(arg_keys[5], 1), 0, LEVELS - 1).astype(jnp.int32)
    trap_table = draw_trap_table(jax.random.fold_in(arg_keys[9], 71), 0)
    mean_field = draw_mean_field(jax.random.fold_in(arg_keys[9], 71), 0)
    pairing = jnp.clip(0.2 + 0.8 * jax.random.uniform(arg_keys[8], (NZ, NY * NX), jnp.float32) ** shard_levels(arg_keys[8], (NZ, NY * NX), ((0, 16),), -0.2, 0.2), 0.2, 1.0)
    return {"quasi": quasi, "counts": counts, "slot_slice": slot_slice, "occupation": occupation, "filter_coef": filter_coef, "trap_index": trap_index, "trap_table": trap_table, "mean_field": mean_field, "pairing": pairing}


spectral_scale = 8.5
beta_coef = 0.6
chem_level = 1.0
coupling = 1.0
density_floor = 0.05


def combine(field, zpadded, ypadded, potential, pairing):
    column = jnp.arange(field.shape[-1]) % NX
    left_ok = (column > 0).astype(jnp.float32)
    right_ok = (column < NX - 1).astype(jnp.float32)
    xpadded = jnp.pad(field, ((0, 0), (0, 0), (0, 0), (1, 1)))
    beside_all = zpadded[:, :, 2:] + zpadded[:, :, :-2]
    beside_all = beside_all + ypadded[..., 2 * NX:] + ypadded[..., :-2 * NX]
    beside_all = beside_all + xpadded[..., 2:] * right_ok + xpadded[..., :-2] * left_ok
    single = 0.5 * (6.0 * field - beside_all) + potential * field
    upper = single[0] + pairing * field[1]
    lower = pairing * field[0] - single[1]
    return jnp.stack([upper, lower]) / spectral_scale


def apply_block(field, potential, pairing):
    zpadded = jnp.pad(field, ((0, 0), (0, 0), (1, 1), (0, 0)))
    ypadded = jnp.pad(field, ((0, 0), (0, 0), (0, 0), (NX, NX)))
    return combine(field, zpadded, ypadded, potential, pairing)


def chebyshev(vectors, coefs, operator):
    previous = vectors
    current = operator(vectors)
    filtered = coefs[:, 0][None, :, None, None] * previous + coefs[:, 1][None, :, None, None] * current
    for order in range(2, DEGREE + 1):
        following = 2.0 * operator(current) - previous
        filtered = filtered + coefs[:, order][None, :, None, None] * following
        previous, current = current, following
    return filtered


def reference(quasi, counts, slot_slice, occupation, filter_coef, trap_index, trap_table, mean_field, pairing):
    potential = trap_table[trap_index] + mean_field
    slot_ids = jnp.arange(SLOTS).astype(jnp.int32)
    live = ((slot_ids % CAP) < counts[slot_ids // CAP]).astype(jnp.float32)
    weights = occupation * live
    coefs = filter_coef[slot_slice]

    def operator(field):
        return apply_block(field, potential, pairing)

    def step(carry, device):
        start = (device * CAP).astype(jnp.int32)
        block = lax.dynamic_slice_in_dim(quasi, start, CAP, 1).astype(jnp.float32)
        block_coefs = lax.dynamic_slice_in_dim(coefs, start, CAP, 0)
        block_weights = lax.dynamic_slice_in_dim(weights, start, CAP, 0)
        filtered = chebyshev(block, block_coefs, operator)
        normal = jnp.sum(block_weights[:, None, None] * filtered[1] * filtered[1], axis=0)
        anomal = jnp.sum(block_weights[:, None, None] * filtered[0] * filtered[1], axis=0)
        return carry + jnp.stack([normal, anomal]), None

    start_sums = jnp.zeros((2, NZ, NY * NX), jnp.float32)
    sums, unused = lax.scan(step, start_sums, jnp.arange(N_CUTS).astype(jnp.int32))
    normal_density = sums[0]
    anomalous_density = sums[1]
    cube_root = jnp.cbrt(normal_density + density_floor)
    new_mean_field = 0.5 * mean_field + 0.5 * (beta_coef * cube_root * cube_root - chem_level)
    new_pairing = 0.5 * pairing - coupling * anomalous_density
    return normal_density, anomalous_density, new_mean_field, new_pairing
```

```python
import jax
import jax.numpy as jnp
from jax import lax
from jax.experimental import pallas as pl
from jax.experimental.pallas import tpu as pltpu
from jax.sharding import PartitionSpec as P

NX = 96
DEGREE = 8
CAP = 6
LANES = 128

spectral_scale = 8.5
beta_coef = 0.6
chem_level = 1.0
coupling = 1.0
density_floor = 0.05

PLANES = 16
WINDOWS = 8
TILES = 72
CORE = 9
HALO = 6
SPAN = CORE + 2 * HALO
EXTRA = 6
MESSAGE = SPAN + EXTRA


def pack_kernel(quasi_ref, index_ref, mean_ref, pairing_ref, table_ref, out_ref, rows_ref, pot_ref):
    index = index_ref[...]
    looked = jnp.zeros(index.shape, jnp.float32)
    for level in range(table_ref.shape[0]):
        looked = jnp.where(index == level, table_ref[level], looked)
    potential = looked + mean_ref[...]
    high = potential.astype(jnp.bfloat16).astype(jnp.float32)
    pot_ref[0] = high
    pot_ref[1] = potential - high
    for group in range(2):
        for slot in range(3):
            pair = quasi_ref[3 * group + slot].astype(jnp.float32)
            rows_ref[group, slot : slot + 1, :] = pair[0:1]
            rows_ref[group, 4 + slot : 5 + slot, :] = pair[1:2]
        for tile in range(TILES):
            lanes = slice(tile * LANES, (tile + 1) * LANES)
            rows_ref[group, 3:4, lanes] = pot_ref[0, tile : tile + 1, :]
            rows_ref[group, 7:8, lanes] = pot_ref[1, tile : tile + 1, :]
    for window in range(WINDOWS):
        first = CORE * window - HALO
        begin, end = max(first, 0), min(first + SPAN, TILES)
        for group in range(2):
            slab = 2 * window + group
            if begin > first:
                out_ref[slab, :, : (begin - first) * LANES] = jnp.zeros(
                    (8, (begin - first) * LANES), jnp.bfloat16
                )
            if end < first + SPAN:
                out_ref[slab, :, (end - first) * LANES : SPAN * LANES] = jnp.zeros(
                    (8, (first + SPAN - end) * LANES), jnp.bfloat16
                )
            out_ref[slab, :, (begin - first) * LANES : (end - first) * LANES] = rows_ref[
                group, :, begin * LANES : end * LANES
            ].astype(jnp.bfloat16)
        for extra in range(EXTRA):
            start = first + 4 * extra
            pieces = []
            low, top = max(start, 0), min(start + 4, TILES)
            if low >= top:
                values = jnp.zeros((4, LANES), jnp.float32)
            else:
                values = pairing_ref[low:top, :]
                if low > start:
                    values = jnp.concatenate(
                        [jnp.zeros((low - start, LANES), jnp.float32), values], axis=0
                    )
                if top < start + 4:
                    values = jnp.concatenate(
                        [values, jnp.zeros((start + 4 - top, LANES), jnp.float32)], axis=0
                    )
            upper = values.astype(jnp.bfloat16).astype(jnp.float32)
            tile = jnp.concatenate([upper, values - upper], axis=0).astype(jnp.bfloat16)
            lanes = slice((SPAN + extra) * LANES, (SPAN + extra + 1) * LANES)
            out_ref[2 * window, :, lanes] = tile
            out_ref[2 * window + 1, :, lanes] = tile


def filter_kernel(
    msg_ref, counts_ref, slice_ref, occupation_ref, coef_ref, out_ref, a_ref, c_ref, one_ref, two_ref, acc_ref
):
    cut = lax.axis_index("cuts")
    slab = lax.axis_index("slab")
    group = slab % 2
    window = slab // 2
    row = lax.broadcasted_iota(jnp.int32, (8, LANES), 0)
    lane = lax.broadcasted_iota(jnp.int32, (8, LANES), 1)
    vector = row % 4
    sign = jnp.where(row < 4, 1.0, -1.0).astype(jnp.float32)
    scale = 2.0 / spectral_scale

    base = cut * CAP + group * 3
    coefs = [jnp.zeros((8, LANES), jnp.float32) for _ in range(DEGREE + 1)]
    weight = jnp.zeros((8, LANES), jnp.float32)
    live = counts_ref[cut]
    for slot in range(3):
        mine = vector == slot
        which = slice_ref[base + slot]
        for order in range(DEGREE + 1):
            coefs[order] = jnp.where(mine, coef_ref[which, order], coefs[order])
        alive = jnp.where(group * 3 + slot < live, occupation_ref[base + slot], 0.0)
        weight = jnp.where(mine, alive, weight)

    below_ok = jnp.where(window > 0, 1.0, 0.0)
    above_ok = jnp.where(window < WINDOWS - 1, 1.0, 0.0)

    def inside(tile):
        if tile < HALO:
            return below_ok
        if tile >= HALO + CORE:
            return above_ok
        return None

    hop = sign * (0.5 * scale)
    hops = [hop * below_ok, hop, hop * above_ok]

    def hop_of(tile):
        return hops[0] if tile < HALO else hops[2] if tile >= HALO + CORE else hops[1]

    blank = jnp.zeros((8, SPAN * LANES), jnp.float32)
    for ref in (one_ref, two_ref):
        ref[0] = blank
        ref[PLANES + 1] = blank

    def prepare(z, carry):
        for extra in range(EXTRA):
            fields = msg_ref[z, :, (SPAN + extra) * LANES : (SPAN + extra + 1) * LANES].astype(jnp.float32)
            for part in range(4):
                tile = 4 * extra + part
                if tile >= SPAN:
                    continue
                lanes = slice(tile * LANES, (tile + 1) * LANES)
                block = msg_ref[z, :, lanes].astype(jnp.float32)
                pairing = fields[part : part + 1] + fields[part + 4 : part + 5]
                potential = block[3:4] + block[7:8]
                onsite = (potential + 3.0) * scale
                cross = pairing * scale
                ok = inside(tile)
                if ok is not None:
                    onsite = onsite * ok
                    cross = cross * ok
                a_ref[z, :, lanes] = sign * onsite
                c_ref[z, :, lanes] = jnp.broadcast_to(cross, (8, LANES))
                one_ref[z + 1, :, lanes] = jnp.where(vector < 3, block, 0.0)
        return carry

    lax.fori_loop(0, PLANES, prepare, 0)

    def tile_of(ref, z, tile):
        return ref[z, :, tile * LANES : (tile + 1) * LANES]

    def step(order, current_ref, other_ref):
        first = (96 * order) // LANES
        last = SPAN - 1 - first
        if order == DEGREE:
            first, last = HALO, HALO + CORE - 1

        def plane(z, carry):
            middles, lefts, rights, befores, afters = {}, {}, {}, {}, {}
            for tile in range(max(first - 1, 0), min(last + 1, SPAN - 1) + 1):
                value = tile_of(current_ref, z + 1, tile)
                middles[tile] = value
                lefts[tile] = pltpu.roll(value, 1, 1)
                rights[tile] = pltpu.roll(value, LANES - 1, 1)
                befores[tile] = pltpu.roll(value, 96, 1)
                afters[tile] = pltpu.roll(value, 32, 1)
            for tile in range(first, last + 1):
                previous = max(tile - 1, 0)
                following = min(tile + 1, SPAN - 1)
                kind = tile % 3
                if kind == 0:
                    left = jnp.where((lane == 0) | (lane == 96), 0.0, lefts[tile])
                    right = jnp.where(lane == 127, rights[following], rights[tile])
                    right = jnp.where(lane == 95, 0.0, right)
                elif kind == 1:
                    left = jnp.where(lane == 0, lefts[previous], lefts[tile])
                    left = jnp.where(lane == 64, 0.0, left)
                    right = jnp.where(lane == 127, rights[following], rights[tile])
                    right = jnp.where(lane == 63, 0.0, right)
                else:
                    left = jnp.where(lane == 0, lefts[previous], lefts[tile])
                    left = jnp.where(lane == 32, 0.0, left)
                    right = jnp.where((lane == 31) | (lane == 127), 0.0, rights[tile])
                before = jnp.where(lane < 96, befores[previous], befores[tile])
                after = jnp.where(lane < 32, afters[tile], afters[following])
                beside = (left + right) + (before + after)
                beside = beside + (tile_of(current_ref, z, tile) + tile_of(current_ref, z + 2, tile))
                middle = middles[tile]
                swapped = pltpu.roll(middle, 4, 0)
                result = (
                    tile_of(a_ref, z, tile) * middle
                    + tile_of(c_ref, z, tile) * swapped
                    - hop_of(tile) * beside
                )
                if order == 1:
                    result = 0.5 * result
                else:
                    result = result - tile_of(other_ref, z + 1, tile)
                if order < DEGREE:
                    other_ref[z + 1, :, tile * LANES : (tile + 1) * LANES] = result
                if HALO <= tile < HALO + CORE:
                    core = slice((tile - HALO) * LANES, (tile - HALO + 1) * LANES)
                    if order == 1:
                        total = coefs[0] * middle + coefs[1] * result
                    else:
                        total = acc_ref[z, :, core] + coefs[order] * result
                    if order < DEGREE:
                        acc_ref[z, :, core] = total
                    else:
                        mixed = jnp.where(row < 4, pltpu.roll(total, 4, 0), total) * total
                        mixed = mixed * weight
                        mixed = mixed + pltpu.roll(mixed, 7, 0)
                        mixed = mixed + pltpu.roll(mixed, 6, 0)
                        acc_ref[z, :, core] = mixed
            if order == DEGREE:
                normal = acc_ref[z, 4:5, :]
                anomalous = acc_ref[z, 0:1, :]
                for half in range(2):
                    sites = slice(half * 576, half * 576 + 576)
                    out_ref[2 * z + half, 0:1, :] = normal[:, sites]
                    out_ref[2 * z + half, 1:2, :] = anomalous[:, sites]
            return carry

        lax.fori_loop(0, PLANES, plane, 0)

    for order in range(1, DEGREE + 1):
        if order % 2 == 1:
            step(order, one_ref, two_ref)
        else:
            step(order, two_ref, one_ref)


def sum_kernel(parts_ref, first_ref, second_ref):
    group = lax.axis_index("slab") % 2
    total = jnp.sum(parts_ref[...], axis=0)
    near, far = total[:, :288], total[:, 288:]
    first_ref[...] = jnp.where(group == 0, near, far)
    second_ref[...] = jnp.where(group == 0, far, near)


def vmem(count):
    return [pl.BlockSpec(memory_space=pltpu.VMEM)] * count


def smem(count):
    return [pl.BlockSpec(memory_space=pltpu.SMEM)] * count


def routes(flip):
    pairs = []
    for cut in range(32):
        for slab in range(16):
            group, window = slab % 2, slab // 2
            part = group ^ flip
            pairs.append((cut * 16 + slab, (4 * window + 2 * (cut % 2) + part) * 16 + cut // 2))
    return pairs


def body(
    quasi, counts, slot_slice, occupation, filter_coef, trap_index, trap_table, mean_field, pairing
):
    share = mean_field.shape[1] // lax.axis_size("cuts")
    packed = jnp.transpose(quasi, (1, 2, 0, 3)).reshape(CAP, 2, TILES * LANES)
    message = pl.pallas_call(
        pack_kernel,
        out_shape=jax.ShapeDtypeStruct((PLANES, 8, MESSAGE * LANES), jnp.bfloat16),
        in_specs=vmem(4) + smem(1),
        out_specs=pl.BlockSpec(memory_space=pltpu.VMEM),
        scratch_shapes=[
            pltpu.VMEM((2, 8, TILES * LANES), jnp.float32),
            pltpu.VMEM((2, TILES, LANES), jnp.float32),
        ],
        name="pack",
    )(
        packed,
        trap_index.reshape(TILES, LANES),
        mean_field.reshape(TILES, LANES),
        pairing.reshape(TILES, LANES),
        trap_table,
    )
    message = lax.all_to_all(message, "slab", 0, 0, tiled=True)
    parts = pl.pallas_call(
        filter_kernel,
        out_shape=jax.ShapeDtypeStruct((32, 2, 576), jnp.float32),
        in_specs=vmem(1) + smem(4),
        out_specs=pl.BlockSpec(memory_space=pltpu.VMEM),
        scratch_shapes=[
            pltpu.VMEM((PLANES, 8, SPAN * LANES), jnp.float32),
            pltpu.VMEM((PLANES, 8, SPAN * LANES), jnp.float32),
            pltpu.VMEM((PLANES + 2, 8, SPAN * LANES), jnp.float32),
            pltpu.VMEM((PLANES + 2, 8, SPAN * LANES), jnp.float32),
            pltpu.VMEM((PLANES, 8, CORE * LANES), jnp.float32),
        ],
        name="filter",
    )(message, counts, slot_slice, occupation, filter_coef)
    parts = lax.all_to_all(parts, "cuts", 0, 0, tiled=True)
    first, second = pl.pallas_call(
        sum_kernel,
        out_shape=[jax.ShapeDtypeStruct((2, 288), jnp.float32)] * 2,
        in_specs=vmem(1),
        out_specs=vmem(2),
        name="total",
    )(parts)
    first = lax.ppermute(first, ("cuts", "slab"), routes(0))
    second = lax.ppermute(second, ("cuts", "slab"), routes(1))
    sums = first + second
    offset = lax.axis_index("cuts") * share
    mean_local = lax.dynamic_slice_in_dim(mean_field, offset, share, 1)
    pairing_local = lax.dynamic_slice_in_dim(pairing, offset, share, 1)
    normal_density = sums[0:1]
    anomalous_density = sums[1:2]
    cube_root = jnp.cbrt(normal_density + density_floor)
    new_mean_field = 0.5 * mean_local + 0.5 * (beta_coef * cube_root * cube_root - chem_level)
    new_pairing = 0.5 * pairing_local - coupling * anomalous_density
    return (normal_density, anomalous_density, new_mean_field, new_pairing)


def solution(mesh):
    return jax.shard_map(
        body,
        mesh=mesh,
        in_specs=(
            P(None, "cuts", "slab", None),
            P(),
            P(),
            P(),
            P(),
            P("slab", None),
            P(),
            P("slab", None),
            P("slab", None),
        ),
        out_specs=(P("slab", "cuts"), P("slab", "cuts"), P("slab", "cuts"), P("slab", "cuts")),
        check_vma=False,
    )
```

```python
import jax
import jax.numpy as jnp
from jax import lax
from jax.experimental import pallas as pl
from jax.experimental.pallas import tpu as pltpu
from jax.sharding import PartitionSpec as P

NX = 96
DEGREE = 8
CAP = 6
LANES = 128

spectral_scale = 8.5
beta_coef = 0.6
chem_level = 1.0
coupling = 1.0
density_floor = 0.05

PLANES = 16
WINDOWS = 8
TILES = 72
CORE = 9
HALO = 6
SPAN = CORE + 2 * HALO
EXTRA = 6
MESSAGE = SPAN + EXTRA


def pack_kernel(quasi_ref, index_ref, mean_ref, pairing_ref, table_ref, out_ref, rows_ref, pot_ref):
    index = index_ref[...]
    looked = jnp.zeros(index.shape, jnp.float32)
    for level in range(table_ref.shape[0]):
        looked = jnp.where(index == level, table_ref[level], looked)
    potential = looked + mean_ref[...]
    high = potential.astype(jnp.bfloat16).astype(jnp.float32)
    pot_ref[0] = high
    pot_ref[1] = potential - high
    for group in range(2):
        for slot in range(3):
            pair = quasi_ref[3 * group + slot].astype(jnp.float32)
            rows_ref[group, slot : slot + 1, :] = pair[0:1]
            rows_ref[group, 4 + slot : 5 + slot, :] = pair[1:2]
        for tile in range(TILES):
            lanes = slice(tile * LANES, (tile + 1) * LANES)
            rows_ref[group, 3:4, lanes] = pot_ref[0, tile : tile + 1, :]
            rows_ref[group, 7:8, lanes] = pot_ref[1, tile : tile + 1, :]
    for window in range(WINDOWS):
        first = CORE * window - HALO
        begin, end = max(first, 0), min(first + SPAN, TILES)
        for group in range(2):
            slab = 2 * window + group
            if begin > first:
                out_ref[slab, :, : (begin - first) * LANES] = jnp.zeros(
                    (8, (begin - first) * LANES), jnp.bfloat16
                )
            if end < first + SPAN:
                out_ref[slab, :, (end - first) * LANES : SPAN * LANES] = jnp.zeros(
                    (8, (first + SPAN - end) * LANES), jnp.bfloat16
                )
            out_ref[slab, :, (begin - first) * LANES : (end - first) * LANES] = rows_ref[
                group, :, begin * LANES : end * LANES
            ].astype(jnp.bfloat16)
        for extra in range(EXTRA):
            start = first + 4 * extra
            pieces = []
            low, top = max(start, 0), min(start + 4, TILES)
            if low >= top:
                values = jnp.zeros((4, LANES), jnp.float32)
            else:
                values = pairing_ref[low:top, :]
                if low > start:
                    values = jnp.concatenate(
                        [jnp.zeros((low - start, LANES), jnp.float32), values], axis=0
                    )
                if top < start + 4:
                    values = jnp.concatenate(
                        [values, jnp.zeros((start + 4 - top, LANES), jnp.float32)], axis=0
                    )
            upper = values.astype(jnp.bfloat16).astype(jnp.float32)
            tile = jnp.concatenate([upper, values - upper], axis=0).astype(jnp.bfloat16)
            lanes = slice((SPAN + extra) * LANES, (SPAN + extra + 1) * LANES)
            out_ref[2 * window, :, lanes] = tile
            out_ref[2 * window + 1, :, lanes] = tile


ROWS = 28
OWN = 12
STRIDE = 24
BLOCK = ROWS * STRIDE


def filter_kernel(
    msg_ref, counts_ref, slice_ref, occupation_ref, coef_ref, keep_ref, send_ref,
    one_ref, two_ref, a_ref, c_ref, acc_ref, density_ref,
):
    cut = lax.axis_index("cuts")
    slab = lax.axis_index("slab")
    group = slab % 2
    window = slab // 2
    scale = 2.0 / spectral_scale
    lane = lax.broadcasted_iota(jnp.int32, (8, LANES), 1)
    below_ok = jnp.where(window > 0, 1.0, 0.0)
    above_ok = jnp.where(window < WINDOWS - 1, 1.0, 0.0)
    on_row = jnp.where(lane < NX, 1.0, 0.0).astype(jnp.float32)
    inside = [on_row * below_ok, on_row, on_row * above_ok]

    def place(y):
        return 0 if y < 8 else 1 if y < 8 + OWN else 2

    hops = [mask * (0.5 * scale) for mask in inside]

    def chosen(count, pick):
        out = lax.broadcasted_iota(jnp.int32, (count, LANES), 0)
        source = lax.broadcasted_iota(jnp.int32, (count, LANES), 1)
        same = (out % PLANES) == (source // 8)
        return jnp.where(same & pick(out // PLANES, source % 8), 1.0, 0.0).astype(jnp.bfloat16)

    gather = chosen(
        7 * PLANES,
        lambda i, row: (row == (i // 3) * 4 + i % 3) | ((i == 6) & (row % 4 == 3)),
    )
    spread = chosen(4 * PLANES, lambda part, row: row % 4 == part)

    for ref in (one_ref, two_ref):
        for block in range(6 * ROWS + 1):
            ref[block * STRIDE : block * STRIDE + 8, :] = jnp.zeros((8, LANES), jnp.float32)
    density_ref[...] = jnp.zeros_like(density_ref)

    def unpack(tiles):
        first, second, third = tiles
        wide = lax.broadcasted_iota(jnp.int32, first.shape, 1)
        ok = wide < NX
        rows = [
            first,
            jnp.where(wide < 32, pltpu.roll(first, 32, 1), pltpu.roll(second, 32, 1)),
            jnp.where(wide < 64, pltpu.roll(second, 64, 1), pltpu.roll(third, 64, 1)),
            pltpu.roll(third, 96, 1),
        ]
        return [jnp.where(ok, row, 0.0) for row in rows]

    fields = []
    for extra in range(EXTRA):
        lanes = slice((SPAN + extra) * LANES, (SPAN + extra + 1) * LANES)
        part = jnp.dot(spread, msg_ref[:, lanes], preferred_element_type=jnp.float32)
        fields += [part[16 * k : 16 * k + 16] for k in range(4)]
    for quad in range(ROWS // 4):
        lanes = slice(3 * quad * LANES, 3 * (quad + 1) * LANES)
        taken = jnp.dot(gather, msg_ref[:, lanes], preferred_element_type=jnp.float32)
        rows = unpack([taken[:, k * LANES : (k + 1) * LANES] for k in range(3)])
        pairs = unpack(fields[3 * quad : 3 * quad + 3])
        for k in range(4):
            y = 4 * quad + k
            mask = inside[place(y)]
            for i in range(6):
                base = i * BLOCK + y * STRIDE + 8
                one_ref[base : base + 16, :] = rows[k][16 * i : 16 * i + 16]
            for high in range(2):
                at = slice(16 * y + 8 * high, 16 * y + 8 * high + 8)
                a_ref[at, :] = (rows[k][96 + 8 * high : 104 + 8 * high] + 3.0) * (mask * scale)
                c_ref[at, :] = pairs[k][8 * high : 8 * high + 8] * (mask * scale)

    live = counts_ref[cut]
    start = cut * CAP + group * 3

    def vector(slot, carry):
        which = slice_ref[start + slot]
        weight = jnp.where(group * 3 + slot < live, occupation_ref[start + slot], 0.0)
        coefs = [coef_ref[which, order] for order in range(DEGREE + 1)]
        shift = slot * BLOCK

        def load(ref, comp, y, offset):
            origin = pl.multiple_of(shift + comp * 3 * BLOCK, 8)
            return ref[pl.ds(origin + y * STRIDE + 8 + offset, 8), :]

        for order in range(1, DEGREE + 1):
            now, other = (one_ref, two_ref) if order % 2 == 1 else (two_ref, one_ref)
            for y in range(order, ROWS - order):
                hop = hops[place(y)]
                for high in range(2):
                    z = 8 * high
                    onsite = a_ref[16 * y + z : 16 * y + z + 8, :]
                    cross = c_ref[16 * y + z : 16 * y + z + 8, :]
                    middles, singles = [], []
                    for comp in range(2):
                        middle = load(now, comp, y, z)
                        beside = pltpu.roll(middle, 1, 1) + pltpu.roll(middle, LANES - 1, 1)
                        beside = beside + (load(now, comp, y - 1, z) + load(now, comp, y + 1, z))
                        beside = beside + (load(now, comp, y, z - 1) + load(now, comp, y, z + 1))
                        middles.append(middle)
                        singles.append(onsite * middle - hop * beside)
                    results = [
                        singles[0] + cross * middles[1],
                        cross * middles[0] - singles[1],
                    ]
                    totals = []
                    for comp in range(2):
                        result = results[comp]
                        if order == 1:
                            result = 0.5 * result
                        else:
                            result = result - load(other, comp, y, z)
                        if order < DEGREE:
                            origin = pl.multiple_of(shift + comp * 3 * BLOCK, 8)
                            other[pl.ds(origin + y * STRIDE + 8 + z, 8), :] = result
                        if 8 <= y < 8 + OWN:
                            at = (comp * OWN + y - 8) * 16 + z
                            if order == 1:
                                total = coefs[0] * middles[comp] + coefs[1] * result
                            else:
                                total = acc_ref[at : at + 8, :] + coefs[order] * result
                            if order < DEGREE:
                                acc_ref[at : at + 8, :] = total
                            totals.append(total)
                    if order == DEGREE:
                        weighted = weight * totals[1]
                        at = (y - 8) * 16 + z
                        density_ref[at : at + 8, :] += weighted * totals[1]
                        at = at + OWN * 16
                        density_ref[at : at + 8, :] += weighted * totals[0]
        return carry

    lax.fori_loop(0, 3, vector, 0)

    for density in range(2):
        for y in range(OWN):
            quarter, row = y // 3, y % 3
            lanes = slice((3 * density + row) * LANES, (3 * density + row + 1) * LANES)
            at = (density * OWN + y) * 16
            first, second = density_ref[at : at + 8, :], density_ref[at + 8 : at + 16, :]
            mine = group == 0
            keep_ref[8 * quarter : 8 * quarter + 8, lanes] = jnp.where(mine, first, second)
            send_ref[8 * quarter : 8 * quarter + 8, lanes] = jnp.where(mine, second, first)


def join_kernel(keep_ref, got_ref, out_ref):
    total = keep_ref[...] + got_ref[...]
    for piece in range(32):
        out_ref[piece] = total[piece : piece + 1]


def sum_kernel(parts_ref, out_ref):
    total = jnp.sum(parts_ref[...], axis=0)
    lane = lax.broadcasted_iota(jnp.int32, (1, LANES), 1)
    for density in range(2):
        first, second, third = [
            total[:, (3 * density + k) * LANES : (3 * density + k + 1) * LANES] for k in range(3)
        ]
        second, third = pltpu.roll(second, 96, 1), pltpu.roll(third, 64, 1)
        row = slice(density, density + 1)
        out_ref[row, 0:128] = jnp.where(lane < 96, first, second)
        out_ref[row, 128:256] = jnp.where(lane < 64, second, third)
        out_ref[row, 256:288] = third[:, :32]


def vmem(count):
    return [pl.BlockSpec(memory_space=pltpu.VMEM)] * count


def smem(count):
    return [pl.BlockSpec(memory_space=pltpu.SMEM)] * count


def filter_call(message, counts, slot_slice, occupation, filter_coef):
    return pl.pallas_call(
        filter_kernel,
        out_shape=[jax.ShapeDtypeStruct((32, 6 * LANES), jnp.float32)] * 2,
        in_specs=vmem(1) + smem(4),
        out_specs=vmem(2),
        scratch_shapes=[
            pltpu.VMEM((6 * BLOCK + 8, LANES), jnp.float32),
            pltpu.VMEM((6 * BLOCK + 8, LANES), jnp.float32),
            pltpu.VMEM((16 * ROWS, LANES), jnp.float32),
            pltpu.VMEM((16 * ROWS, LANES), jnp.float32),
            pltpu.VMEM((2 * OWN * 16, LANES), jnp.float32),
            pltpu.VMEM((2 * OWN * 16, LANES), jnp.float32),
        ],
        name="filter",
    )(message.reshape(8 * PLANES, MESSAGE * LANES), counts, slot_slice, occupation, filter_coef)


def partners():
    return [(slab, slab ^ 1) for slab in range(16)]


def routes():
    pairs = []
    for cut in range(32):
        for slab in range(16):
            group, window = slab % 2, slab // 2
            target = (4 * window + cut // 8) * 16 + 8 * group + cut % 8
            pairs.append((cut * 16 + slab, target))
    return pairs


def body(
    quasi, counts, slot_slice, occupation, filter_coef, trap_index, trap_table, mean_field, pairing
):
    share = mean_field.shape[1] // lax.axis_size("cuts")
    packed = jnp.transpose(quasi, (1, 2, 0, 3)).reshape(CAP, 2, TILES * LANES)
    message = pl.pallas_call(
        pack_kernel,
        out_shape=jax.ShapeDtypeStruct((PLANES, 8, MESSAGE * LANES), jnp.bfloat16),
        in_specs=vmem(4) + smem(1),
        out_specs=pl.BlockSpec(memory_space=pltpu.VMEM),
        scratch_shapes=[
            pltpu.VMEM((2, 8, TILES * LANES), jnp.float32),
            pltpu.VMEM((2, TILES, LANES), jnp.float32),
        ],
        name="pack",
    )(
        packed,
        trap_index.reshape(TILES, LANES),
        mean_field.reshape(TILES, LANES),
        pairing.reshape(TILES, LANES),
        trap_table,
    )
    message = lax.all_to_all(message, "slab", 0, 0, tiled=True)
    keep, send = filter_call(message, counts, slot_slice, occupation, filter_coef)
    got = lax.ppermute(send, "slab", partners())
    parts = pl.pallas_call(
        join_kernel,
        out_shape=jax.ShapeDtypeStruct((32, 1, 6 * LANES), jnp.float32),
        in_specs=vmem(2),
        out_specs=pl.BlockSpec(memory_space=pltpu.VMEM),
        name="join",
    )(keep, got)
    parts = lax.all_to_all(parts, "cuts", 0, 0, tiled=True)
    sums = pl.pallas_call(
        sum_kernel,
        out_shape=jax.ShapeDtypeStruct((2, 288), jnp.float32),
        in_specs=vmem(1),
        out_specs=pl.BlockSpec(memory_space=pltpu.VMEM),
        name="total",
    )(parts)
    sums = lax.ppermute(sums, ("cuts", "slab"), routes())
    offset = lax.axis_index("cuts") * share
    mean_local = lax.dynamic_slice_in_dim(mean_field, offset, share, 1)
    pairing_local = lax.dynamic_slice_in_dim(pairing, offset, share, 1)
    normal_density = sums[0:1]
    anomalous_density = sums[1:2]
    cube_root = jnp.cbrt(normal_density + density_floor)
    new_mean_field = 0.5 * mean_local + 0.5 * (beta_coef * cube_root * cube_root - chem_level)
    new_pairing = 0.5 * pairing_local - coupling * anomalous_density
    return (normal_density, anomalous_density, new_mean_field, new_pairing)


def solution(mesh):
    return jax.shard_map(
        body,
        mesh=mesh,
        in_specs=(
            P(None, "cuts", "slab", None),
            P(),
            P(),
            P(),
            P(),
            P("slab", None),
            P(),
            P("slab", None),
            P("slab", None),
        ),
        out_specs=(P("slab", "cuts"), P("slab", "cuts"), P("slab", "cuts"), P("slab", "cuts")),
        check_vma=False,
    )
```

```python
import jax
import jax.numpy as jnp
from jax import lax
from jax.experimental import pallas as pl
from jax.experimental.pallas import tpu as pltpu
from jax.sharding import PartitionSpec as P

NX = 96
DEGREE = 8
CAP = 6
LANES = 128

spectral_scale = 8.5
beta_coef = 0.6
chem_level = 1.0
coupling = 1.0
density_floor = 0.05

PLANES = 16
WINDOWS = 8
TILES = 72
CORE = 9
QUAD = 4 * LANES
MESSAGE = 3 * QUAD
HALO = 2 * QUAD


def slab_of(group, window):
    return (window // 2) * 4 + group * 2 + window % 2


def pack_kernel(quasi_ref, index_ref, mean_ref, pairing_ref, table_ref, out_ref, rows_ref, pot_ref):
    index = index_ref[...]
    looked = jnp.zeros(index.shape, jnp.float32)
    for level in range(table_ref.shape[0]):
        looked = jnp.where(index == level, table_ref[level], looked)
    potential = looked + mean_ref[...]
    high = potential.astype(jnp.bfloat16).astype(jnp.float32)
    pot_ref[0] = high
    pot_ref[1] = potential - high
    for group in range(2):
        for slot in range(3):
            pair = quasi_ref[3 * group + slot].astype(jnp.float32)
            rows_ref[group, slot : slot + 1, :] = pair[0:1]
            rows_ref[group, 4 + slot : 5 + slot, :] = pair[1:2]
        for tile in range(TILES):
            lanes = slice(tile * LANES, (tile + 1) * LANES)
            rows_ref[group, 3:4, lanes] = pot_ref[0, tile : tile + 1, :]
            rows_ref[group, 7:8, lanes] = pot_ref[1, tile : tile + 1, :]
    for window in range(WINDOWS):
        for quad in range(3):
            first = CORE * window + 3 * quad
            values = jnp.concatenate(
                [pairing_ref[first : first + 3, :], jnp.zeros((1, LANES), jnp.float32)], axis=0
            )
            upper = values.astype(jnp.bfloat16).astype(jnp.float32)
            extra = jnp.concatenate([upper, values - upper], axis=0).astype(jnp.bfloat16)
            start = quad * QUAD
            for group in range(2):
                slab = slab_of(group, window)
                out_ref[slab, :, start : start + 3 * LANES] = rows_ref[
                    group, :, first * LANES : (first + 3) * LANES
                ].astype(jnp.bfloat16)
                out_ref[slab, :, start + 3 * LANES : start + QUAD] = extra


ROWS = 28
OWN = 12
STRIDE = 24
BLOCK = ROWS * STRIDE


def filter_kernel(
    low_ref, own_ref, high_ref, counts_ref, slice_ref, occupation_ref, coef_ref, out_ref,
    one_ref, two_ref, a_ref, c_ref, acc_ref, density_ref,
):
    cut = lax.axis_index("cuts")
    slab = lax.axis_index("slab")
    group = (slab // 2) % 2
    window = (slab // 4) * 2 + slab % 2
    scale = 2.0 / spectral_scale
    lane = lax.broadcasted_iota(jnp.int32, (8, LANES), 1)
    below_ok = jnp.where(window > 0, 1.0, 0.0)
    above_ok = jnp.where(window < WINDOWS - 1, 1.0, 0.0)
    on_row = jnp.where(lane < NX, 1.0, 0.0).astype(jnp.float32)
    inside = [on_row * below_ok, on_row, on_row * above_ok]

    def place(y):
        return 0 if y < 8 else 1 if y < 8 + OWN else 2

    hops = [mask * (0.5 * scale) for mask in inside]

    def chosen(count, pick):
        out = lax.broadcasted_iota(jnp.int32, (count, LANES), 0)
        source = lax.broadcasted_iota(jnp.int32, (count, LANES), 1)
        same = (out % PLANES) == (source // 8)
        return jnp.where(same & pick(out // PLANES, source % 8), 1.0, 0.0).astype(jnp.bfloat16)

    gather = chosen(
        7 * PLANES,
        lambda i, row: (row == (i // 3) * 4 + i % 3) | ((i == 6) & (row % 4 == 3)),
    )
    spread = chosen(3 * PLANES, lambda part, row: row % 4 == part)

    for ref in (one_ref, two_ref):
        for block in range(6 * ROWS + 1):
            ref[block * STRIDE : block * STRIDE + 8, :] = jnp.zeros((8, LANES), jnp.float32)
    density_ref[...] = jnp.zeros_like(density_ref)

    def unpack(tiles):
        first, second, third = tiles
        wide = lax.broadcasted_iota(jnp.int32, first.shape, 1)
        ok = wide < NX
        rows = [
            first,
            jnp.where(wide < 32, pltpu.roll(first, 32, 1), pltpu.roll(second, 32, 1)),
            jnp.where(wide < 64, pltpu.roll(second, 64, 1), pltpu.roll(third, 64, 1)),
            pltpu.roll(third, 96, 1),
        ]
        return [jnp.where(ok, row, 0.0) for row in rows]

    for quad in range(ROWS // 4):
        if quad < 2:
            ref, start = low_ref, quad * QUAD
        elif quad < 5:
            ref, start = own_ref, (quad - 2) * QUAD
        else:
            ref, start = high_ref, (quad - 5) * QUAD
        taken = jnp.dot(
            gather, ref[:, start : start + 3 * LANES], preferred_element_type=jnp.float32
        )
        part = jnp.dot(
            spread, ref[:, start + 3 * LANES : start + QUAD], preferred_element_type=jnp.float32
        )
        rows = unpack([taken[:, k * LANES : (k + 1) * LANES] for k in range(3)])
        pairs = unpack([part[16 * k : 16 * k + 16] for k in range(3)])
        for k in range(4):
            y = 4 * quad + k
            mask = inside[place(y)]
            for i in range(6):
                base = i * BLOCK + y * STRIDE + 8
                one_ref[base : base + 16, :] = rows[k][16 * i : 16 * i + 16]
            for high in range(2):
                at = slice(16 * y + 8 * high, 16 * y + 8 * high + 8)
                a_ref[at, :] = (rows[k][96 + 8 * high : 104 + 8 * high] + 3.0) * (mask * scale)
                c_ref[at, :] = pairs[k][8 * high : 8 * high + 8] * (mask * scale)

    live = counts_ref[cut]
    start = cut * CAP + group * 3

    def vector(slot, carry):
        which = slice_ref[start + slot]
        weight = jnp.where(group * 3 + slot < live, occupation_ref[start + slot], 0.0)
        coefs = [coef_ref[which, order] for order in range(DEGREE + 1)]
        shift = slot * BLOCK

        def load(ref, comp, y, offset):
            origin = pl.multiple_of(shift + comp * 3 * BLOCK, 8)
            return ref[pl.ds(origin + y * STRIDE + 8 + offset, 8), :]

        for order in range(1, DEGREE + 1):
            now, other = (one_ref, two_ref) if order % 2 == 1 else (two_ref, one_ref)
            for y in range(order, ROWS - order):
                hop = hops[place(y)]
                for high in range(2):
                    z = 8 * high
                    onsite = a_ref[16 * y + z : 16 * y + z + 8, :]
                    cross = c_ref[16 * y + z : 16 * y + z + 8, :]
                    middles, singles = [], []
                    for comp in range(2):
                        middle = load(now, comp, y, z)
                        beside = pltpu.roll(middle, 1, 1) + pltpu.roll(middle, LANES - 1, 1)
                        beside = beside + (load(now, comp, y - 1, z) + load(now, comp, y + 1, z))
                        beside = beside + (load(now, comp, y, z - 1) + load(now, comp, y, z + 1))
                        middles.append(middle)
                        singles.append(onsite * middle - hop * beside)
                    results = [
                        singles[0] + cross * middles[1],
                        cross * middles[0] - singles[1],
                    ]
                    totals = []
                    for comp in range(2):
                        result = results[comp]
                        if order == 1:
                            result = 0.5 * result
                        else:
                            result = result - load(other, comp, y, z)
                        if order < DEGREE:
                            origin = pl.multiple_of(shift + comp * 3 * BLOCK, 8)
                            other[pl.ds(origin + y * STRIDE + 8 + z, 8), :] = result
                        if 8 <= y < 8 + OWN:
                            at = (comp * OWN + y - 8) * 16 + z
                            if order == 1:
                                total = coefs[0] * middles[comp] + coefs[1] * result
                            else:
                                total = acc_ref[at : at + 8, :] + coefs[order] * result
                            if order < DEGREE:
                                acc_ref[at : at + 8, :] = total
                            totals.append(total)
                    if order == DEGREE:
                        weighted = weight * totals[1]
                        at = (y - 8) * 16 + z
                        density_ref[at : at + 8, :] += weighted * totals[1]
                        at = at + OWN * 16
                        density_ref[at : at + 8, :] += weighted * totals[0]
        return carry

    lax.fori_loop(0, 3, vector, 0)

    for density in range(2):
        for y in range(OWN):
            lanes = slice((3 * density + y % 3) * LANES, (3 * density + y % 3 + 1) * LANES)
            at = (density * OWN + y) * 16
            for high in range(2):
                values = density_ref[at + 8 * high : at + 8 * high + 8, :]
                for k in range(8):
                    out_ref[piece_of(8 * high + k, y // 3), :, lanes] = values[k : k + 1]


def piece_of(plane, quarter):
    cut = 4 * (2 * (plane // 4) + plane % 2) + quarter
    return 2 * cut + (plane // 2) % 2


def sum_kernel(parts_ref, out_ref):
    total = jnp.sum(parts_ref[...], axis=0)
    lane = lax.broadcasted_iota(jnp.int32, (1, LANES), 1)
    for density in range(2):
        first, second, third = [
            total[:, (3 * density + k) * LANES : (3 * density + k + 1) * LANES] for k in range(3)
        ]
        second, third = pltpu.roll(second, 96, 1), pltpu.roll(third, 64, 1)
        row = slice(density, density + 1)
        out_ref[row, 0:128] = jnp.where(lane < 96, first, second)
        out_ref[row, 128:256] = jnp.where(lane < 64, second, third)
        out_ref[row, 256:288] = third[:, :32]


def vmem(count):
    return [pl.BlockSpec(memory_space=pltpu.VMEM)] * count


def smem(count):
    return [pl.BlockSpec(memory_space=pltpu.SMEM)] * count


def filter_call(low, own, high, counts, slot_slice, occupation, filter_coef):
    flat = [part.reshape(8 * PLANES, part.shape[2]) for part in (low, own, high)]
    return pl.pallas_call(
        filter_kernel,
        out_shape=jax.ShapeDtypeStruct((64, 1, 6 * LANES), jnp.float32),
        in_specs=vmem(3) + smem(4),
        out_specs=pl.BlockSpec(memory_space=pltpu.VMEM),
        scratch_shapes=[
            pltpu.VMEM((6 * BLOCK + 8, LANES), jnp.float32),
            pltpu.VMEM((6 * BLOCK + 8, LANES), jnp.float32),
            pltpu.VMEM((16 * ROWS, LANES), jnp.float32),
            pltpu.VMEM((16 * ROWS, LANES), jnp.float32),
            pltpu.VMEM((2 * OWN * 16, LANES), jnp.float32),
            pltpu.VMEM((2 * OWN * 16, LANES), jnp.float32),
        ],
        name="filter",
    )(*flat, counts, slot_slice, occupation, filter_coef)


def neighbours(by):
    return [
        (slab_of(group, window), slab_of(group, window + by))
        for group in range(2)
        for window in range(WINDOWS)
        if 0 <= window + by < WINDOWS
    ]


def summing_groups():
    return [
        [cut * 16 + slab_of(group, window) for cut in range(32) for group in range(2)]
        for window in range(WINDOWS)
    ]


def routes():
    pairs = []
    for window in range(WINDOWS):
        for plane in range(PLANES):
            for quarter in range(4):
                piece = piece_of(plane, quarter)
                source = (piece // 2) * 16 + slab_of(piece % 2, window)
                pairs.append((source, (4 * window + quarter) * 16 + plane))
    return pairs


def body(
    quasi, counts, slot_slice, occupation, filter_coef, trap_index, trap_table, mean_field, pairing
):
    share = mean_field.shape[1] // lax.axis_size("cuts")
    packed = jnp.transpose(quasi, (1, 2, 0, 3)).reshape(CAP, 2, TILES * LANES)
    message = pl.pallas_call(
        pack_kernel,
        out_shape=jax.ShapeDtypeStruct((PLANES, 8, MESSAGE), jnp.bfloat16),
        in_specs=vmem(4) + smem(1),
        out_specs=pl.BlockSpec(memory_space=pltpu.VMEM),
        scratch_shapes=[
            pltpu.VMEM((2, 8, TILES * LANES), jnp.float32),
            pltpu.VMEM((2, TILES, LANES), jnp.float32),
        ],
        name="pack",
    )(
        packed,
        trap_index.reshape(TILES, LANES),
        mean_field.reshape(TILES, LANES),
        pairing.reshape(TILES, LANES),
        trap_table,
    )
    message = lax.all_to_all(message, "slab", 0, 0, tiled=True)
    low = lax.ppermute(message[:, :, MESSAGE - HALO :], "slab", neighbours(1))
    high = lax.ppermute(message[:, :, :HALO], "slab", neighbours(-1))
    parts = filter_call(low, message, high, counts, slot_slice, occupation, filter_coef)
    parts = lax.all_to_all(
        parts, ("cuts", "slab"), 0, 0, axis_index_groups=summing_groups(), tiled=True
    )
    sums = pl.pallas_call(
        sum_kernel,
        out_shape=jax.ShapeDtypeStruct((2, 288), jnp.float32),
        in_specs=vmem(1),
        out_specs=pl.BlockSpec(memory_space=pltpu.VMEM),
        name="total",
    )(parts)
    sums = lax.ppermute(sums, ("cuts", "slab"), routes())
    offset = lax.axis_index("cuts") * share
    mean_local = lax.dynamic_slice_in_dim(mean_field, offset, share, 1)
    pairing_local = lax.dynamic_slice_in_dim(pairing, offset, share, 1)
    normal_density = sums[0:1]
    anomalous_density = sums[1:2]
    cube_root = jnp.cbrt(normal_density + density_floor)
    new_mean_field = 0.5 * mean_local + 0.5 * (beta_coef * cube_root * cube_root - chem_level)
    new_pairing = 0.5 * pairing_local - coupling * anomalous_density
    return (normal_density, anomalous_density, new_mean_field, new_pairing)


def solution(mesh):
    return jax.shard_map(
        body,
        mesh=mesh,
        in_specs=(
            P(None, "cuts", "slab", None),
            P(),
            P(),
            P(),
            P(),
            P("slab", None),
            P(),
            P("slab", None),
            P("slab", None),
        ),
        out_specs=(P("slab", "cuts"), P("slab", "cuts"), P("slab", "cuts"), P("slab", "cuts")),
        check_vma=False,
    )
```

```python
import jax
import jax.numpy as jnp
from jax import lax
from jax.experimental import pallas as pl
from jax.experimental.pallas import tpu as pltpu
from jax.sharding import PartitionSpec as P

NX = 96
DEGREE = 8
CAP = 6
LANES = 128

spectral_scale = 8.5
beta_coef = 0.6
chem_level = 1.0
coupling = 1.0
density_floor = 0.05

PLANES = 16
WINDOWS = 8
TILES = 72
CORE = 9
QUAD = 4 * LANES
QUADS = 24
SPAN = 7


def slab_of(group, window):
    return (window // 2) * 4 + group * 2 + window % 2


def pack_kernel(
    quasi_ref, index_ref, mean_ref, pairing_ref, table_ref, mine_ref, theirs_ref, rows_ref, pot_ref
):
    half = (lax.axis_index("slab") // 2) % 2
    index = index_ref[...]
    looked = jnp.zeros(index.shape, jnp.float32)
    for level in range(table_ref.shape[0]):
        looked = jnp.where(index == level, table_ref[level], looked)
    potential = looked + mean_ref[...]
    high = potential.astype(jnp.bfloat16).astype(jnp.float32)
    pot_ref[0] = high
    pot_ref[1] = potential - high
    for side, group in ((0, half), (1, 1 - half)):
        for slot in range(3):
            pair = quasi_ref[3 * group + slot].astype(jnp.float32)
            rows_ref[side, slot : slot + 1, :] = pair[0:1]
            rows_ref[side, 4 + slot : 5 + slot, :] = pair[1:2]
        for tile in range(TILES):
            lanes = slice(tile * LANES, (tile + 1) * LANES)
            rows_ref[side, 3:4, lanes] = pot_ref[0, tile : tile + 1, :]
            rows_ref[side, 7:8, lanes] = pot_ref[1, tile : tile + 1, :]
    for quad in range(QUADS):
        first = 3 * quad
        values = jnp.concatenate(
            [pairing_ref[first : first + 3, :], jnp.zeros((1, LANES), jnp.float32)], axis=0
        )
        upper = values.astype(jnp.bfloat16).astype(jnp.float32)
        extra = jnp.concatenate([upper, values - upper], axis=0).astype(jnp.bfloat16)
        start = quad * QUAD
        for side, out_ref in ((0, mine_ref), (1, theirs_ref)):
            out_ref[:, start : start + 3 * LANES] = rows_ref[
                side, :, first * LANES : (first + 3) * LANES
            ].astype(jnp.bfloat16)
            out_ref[:, start + 3 * LANES : start + QUAD] = extra


def window_kernel(mine_ref, got_ref, out_ref):
    half = (lax.axis_index("slab") // 2) % 2
    for window in range(WINDOWS):
        first = 3 * window - 2
        begin, end = max(first, 0), min(first + SPAN, QUADS)
        before, after = begin - first, first + SPAN - end
        for ref, place in ((mine_ref, half), (got_ref, 1 - half)):
            if before:
                out_ref[window, place, :, : before * QUAD] = jnp.zeros(
                    (8, before * QUAD), jnp.bfloat16
                )
            if after:
                out_ref[window, place, :, (SPAN - after) * QUAD :] = jnp.zeros(
                    (8, after * QUAD), jnp.bfloat16
                )
            out_ref[window, place, :, before * QUAD : (SPAN - after) * QUAD] = ref[
                :, begin * QUAD : end * QUAD
            ]


ROWS = 28
OWN = 12
STRIDE = 24
BLOCK = ROWS * STRIDE


def filter_kernel(
    msg_ref, counts_ref, slice_ref, occupation_ref, coef_ref, out_ref,
    one_ref, two_ref, a_ref, c_ref, acc_ref, density_ref,
):
    cut = lax.axis_index("cuts")
    slab = lax.axis_index("slab")
    group = (slab // 2) % 2
    window = (slab // 4) * 2 + slab % 2
    scale = 2.0 / spectral_scale
    lane = lax.broadcasted_iota(jnp.int32, (8, LANES), 1)
    below_ok = jnp.where(window > 0, 1.0, 0.0)
    above_ok = jnp.where(window < WINDOWS - 1, 1.0, 0.0)
    on_row = jnp.where(lane < NX, 1.0, 0.0).astype(jnp.float32)
    inside = [on_row * below_ok, on_row, on_row * above_ok]

    def place(y):
        return 0 if y < 8 else 1 if y < 8 + OWN else 2

    hops = [mask * (0.5 * scale) for mask in inside]

    def chosen(count, pick):
        out = lax.broadcasted_iota(jnp.int32, (count, LANES), 0)
        source = lax.broadcasted_iota(jnp.int32, (count, LANES), 1)
        chip, core, half = source // 32, (source // 16) % 2, (source // 8) % 2
        same = (out % PLANES) == 4 * chip + 2 * half + core
        return jnp.where(same & pick(out // PLANES, source % 8), 1.0, 0.0).astype(jnp.bfloat16)

    gather = chosen(
        7 * PLANES,
        lambda i, row: (row == (i // 3) * 4 + i % 3) | ((i == 6) & (row % 4 == 3)),
    )
    spread = chosen(3 * PLANES, lambda part, row: row % 4 == part)

    for ref in (one_ref, two_ref):
        for block in range(6 * ROWS + 1):
            ref[block * STRIDE : block * STRIDE + 8, :] = jnp.zeros((8, LANES), jnp.float32)
    density_ref[...] = jnp.zeros_like(density_ref)

    def unpack(tiles):
        first, second, third = tiles
        wide = lax.broadcasted_iota(jnp.int32, first.shape, 1)
        ok = wide < NX
        rows = [
            first,
            jnp.where(wide < 32, pltpu.roll(first, 32, 1), pltpu.roll(second, 32, 1)),
            jnp.where(wide < 64, pltpu.roll(second, 64, 1), pltpu.roll(third, 64, 1)),
            pltpu.roll(third, 96, 1),
        ]
        return [jnp.where(ok, row, 0.0) for row in rows]

    for quad in range(ROWS // 4):
        start = quad * QUAD
        taken = jnp.dot(
            gather, msg_ref[:, start : start + 3 * LANES], preferred_element_type=jnp.float32
        )
        part = jnp.dot(
            spread, msg_ref[:, start + 3 * LANES : start + QUAD], preferred_element_type=jnp.float32
        )
        rows = unpack([taken[:, k * LANES : (k + 1) * LANES] for k in range(3)])
        pairs = unpack([part[16 * k : 16 * k + 16] for k in range(3)])
        for k in range(4):
            y = 4 * quad + k
            mask = inside[place(y)]
            for i in range(6):
                base = i * BLOCK + y * STRIDE + 8
                one_ref[base : base + 16, :] = rows[k][16 * i : 16 * i + 16]
            for high in range(2):
                at = slice(16 * y + 8 * high, 16 * y + 8 * high + 8)
                a_ref[at, :] = (rows[k][96 + 8 * high : 104 + 8 * high] + 3.0) * (mask * scale)
                c_ref[at, :] = pairs[k][8 * high : 8 * high + 8] * (mask * scale)

    live = counts_ref[cut]
    start = cut * CAP + group * 3

    def vector(slot, carry):
        which = slice_ref[start + slot]
        weight = jnp.where(group * 3 + slot < live, occupation_ref[start + slot], 0.0)
        coefs = [coef_ref[which, order] for order in range(DEGREE + 1)]
        shift = slot * BLOCK

        def load(ref, comp, y, offset):
            origin = pl.multiple_of(shift + comp * 3 * BLOCK, 8)
            return ref[pl.ds(origin + y * STRIDE + 8 + offset, 8), :]

        for order in range(1, DEGREE + 1):
            now, other = (one_ref, two_ref) if order % 2 == 1 else (two_ref, one_ref)
            for y in range(order, ROWS - order):
                hop = hops[place(y)]
                for high in range(2):
                    z = 8 * high
                    onsite = a_ref[16 * y + z : 16 * y + z + 8, :]
                    cross = c_ref[16 * y + z : 16 * y + z + 8, :]
                    middles, singles = [], []
                    for comp in range(2):
                        middle = load(now, comp, y, z)
                        beside = pltpu.roll(middle, 1, 1) + pltpu.roll(middle, LANES - 1, 1)
                        beside = beside + (load(now, comp, y - 1, z) + load(now, comp, y + 1, z))
                        beside = beside + (load(now, comp, y, z - 1) + load(now, comp, y, z + 1))
                        middles.append(middle)
                        singles.append(onsite * middle - hop * beside)
                    results = [
                        singles[0] + cross * middles[1],
                        cross * middles[0] - singles[1],
                    ]
                    totals = []
                    for comp in range(2):
                        result = results[comp]
                        if order == 1:
                            result = 0.5 * result
                        else:
                            result = result - load(other, comp, y, z)
                        if order < DEGREE:
                            origin = pl.multiple_of(shift + comp * 3 * BLOCK, 8)
                            other[pl.ds(origin + y * STRIDE + 8 + z, 8), :] = result
                        if 8 <= y < 8 + OWN:
                            at = (comp * OWN + y - 8) * 16 + z
                            if order == 1:
                                total = coefs[0] * middles[comp] + coefs[1] * result
                            else:
                                total = acc_ref[at : at + 8, :] + coefs[order] * result
                            if order < DEGREE:
                                acc_ref[at : at + 8, :] = total
                            totals.append(total)
                    if order == DEGREE:
                        weighted = weight * totals[1]
                        at = (y - 8) * 16 + z
                        density_ref[at : at + 8, :] += weighted * totals[1]
                        at = at + OWN * 16
                        density_ref[at : at + 8, :] += weighted * totals[0]
        return carry

    lax.fori_loop(0, 3, vector, 0)

    for quarter in range(4):
        for high in range(2):
            at = 48 * quarter + 8 * high
            normal = [density_ref[at + 16 * k : at + 16 * k + 8, :] for k in range(3)]
            at = at + OWN * 16
            other = [density_ref[at + 16 * k : at + 16 * k + 8, :] for k in range(3)]
            second, third = pltpu.roll(normal[1], 96, 1), pltpu.roll(normal[2], 64, 1)
            last = pltpu.roll(other[2], 96, 1)
            tiles = [
                jnp.where(lane < 96, normal[0], second),
                jnp.where(lane < 64, second, third),
                jnp.where(lane < 32, third, pltpu.roll(other[0], 32, 1)),
                jnp.where(lane < 96, other[1], last),
                last[:, :64],
            ]
            for k in range(8):
                piece = piece_of(8 * high + k, quarter)
                for tile, values in enumerate(tiles):
                    lanes = slice(tile * LANES, tile * LANES + values.shape[1])
                    out_ref[piece, :, lanes] = values[k : k + 1]


def piece_of(plane, quarter):
    cut = 4 * (2 * (plane // 4) + plane % 2) + quarter
    return 2 * cut + (plane // 2) % 2


def sum_kernel(parts_ref, out_ref):
    out_ref[...] = jnp.sum(parts_ref[...], axis=0)


def vmem(count):
    return [pl.BlockSpec(memory_space=pltpu.VMEM)] * count


def smem(count):
    return [pl.BlockSpec(memory_space=pltpu.SMEM)] * count


def grant(mebibytes):
    return pltpu.CompilerParams(vmem_limit_bytes=mebibytes << 20)


def filter_call(message, counts, slot_slice, occupation, filter_coef):
    return pl.pallas_call(
        filter_kernel,
        out_shape=jax.ShapeDtypeStruct((64, 1, 2 * 288), jnp.float32),
        in_specs=vmem(1) + smem(4),
        out_specs=pl.BlockSpec(memory_space=pltpu.VMEM),
        scratch_shapes=[
            pltpu.VMEM((6 * BLOCK + 8, LANES), jnp.float32),
            pltpu.VMEM((6 * BLOCK + 8, LANES), jnp.float32),
            pltpu.VMEM((16 * ROWS, LANES), jnp.float32),
            pltpu.VMEM((16 * ROWS, LANES), jnp.float32),
            pltpu.VMEM((2 * OWN * 16, LANES), jnp.float32),
            pltpu.VMEM((2 * OWN * 16, LANES), jnp.float32),
        ],
        compiler_params=grant(16),
        name="filter",
    )(message.reshape(8 * PLANES, SPAN * QUAD), counts, slot_slice, occupation, filter_coef)


def window_groups():
    return [[slab_of(group, window) for window in range(WINDOWS)] for group in range(2)]


def summing_groups():
    return [
        [cut * 16 + slab_of(group, window) for cut in range(32) for group in range(2)]
        for window in range(WINDOWS)
    ]


def routes():
    pairs = []
    for window in range(WINDOWS):
        for plane in range(PLANES):
            for quarter in range(4):
                piece = piece_of(plane, quarter)
                source = (piece // 2) * 16 + slab_of(piece % 2, window)
                pairs.append((source, (4 * window + quarter) * 16 + plane))
    return pairs


def body(
    quasi, counts, slot_slice, occupation, filter_coef, trap_index, trap_table, mean_field, pairing
):
    share = mean_field.shape[1] // lax.axis_size("cuts")
    packed = jnp.transpose(quasi, (1, 2, 0, 3)).reshape(CAP, 2, TILES * LANES)
    mine, theirs = pl.pallas_call(
        pack_kernel,
        out_shape=[jax.ShapeDtypeStruct((8, QUADS * QUAD), jnp.bfloat16)] * 2,
        in_specs=vmem(4) + smem(1),
        out_specs=vmem(2),
        scratch_shapes=[
            pltpu.VMEM((2, 8, TILES * LANES), jnp.float32),
            pltpu.VMEM((2, TILES, LANES), jnp.float32),
        ],
        compiler_params=grant(8),
        name="pack",
    )(
        packed,
        trap_index.reshape(TILES, LANES),
        mean_field.reshape(TILES, LANES),
        pairing.reshape(TILES, LANES),
        trap_table,
    )
    got = lax.ppermute(theirs, "slab", [(slab, slab ^ 2) for slab in range(16)])
    message = pl.pallas_call(
        window_kernel,
        out_shape=jax.ShapeDtypeStruct((WINDOWS, 2, 8, SPAN * QUAD), jnp.bfloat16),
        in_specs=vmem(2),
        out_specs=pl.BlockSpec(memory_space=pltpu.VMEM),
        compiler_params=grant(8),
        name="window",
    )(mine, got)
    message = lax.all_to_all(
        message, "slab", 0, 0, axis_index_groups=window_groups(), tiled=True
    )
    parts = filter_call(message, counts, slot_slice, occupation, filter_coef)
    parts = lax.all_to_all(
        parts, ("cuts", "slab"), 0, 0, axis_index_groups=summing_groups(), tiled=True
    )
    sums = pl.pallas_call(
        sum_kernel,
        out_shape=jax.ShapeDtypeStruct((1, 2 * 288), jnp.float32),
        in_specs=vmem(1),
        out_specs=pl.BlockSpec(memory_space=pltpu.VMEM),
        compiler_params=grant(4),
        name="total",
    )(parts)
    sums = lax.ppermute(sums, ("cuts", "slab"), routes())
    offset = lax.axis_index("cuts") * share
    mean_local = lax.dynamic_slice_in_dim(mean_field, offset, share, 1)
    pairing_local = lax.dynamic_slice_in_dim(pairing, offset, share, 1)
    normal_density = sums[:, :share]
    anomalous_density = sums[:, share:]
    cube_root = jnp.cbrt(normal_density + density_floor)
    new_mean_field = 0.5 * mean_local + 0.5 * (beta_coef * cube_root * cube_root - chem_level)
    new_pairing = 0.5 * pairing_local - coupling * anomalous_density
    return (normal_density, anomalous_density, new_mean_field, new_pairing)


def solution(mesh):
    return jax.shard_map(
        body,
        mesh=mesh,
        in_specs=(
            P(None, "cuts", "slab", None),
            P(),
            P(),
            P(),
            P(),
            P("slab", None),
            P(),
            P("slab", None),
            P("slab", None),
        ),
        out_specs=(P("slab", "cuts"), P("slab", "cuts"), P("slab", "cuts"), P("slab", "cuts")),
        check_vma=False,
    )
```

```python
import jax
import jax.numpy as jnp
from jax import lax
from jax.experimental import pallas as pl
from jax.experimental.pallas import tpu as pltpu
from jax.sharding import PartitionSpec as P

NX = 96
DEGREE = 8
CAP = 6
LANES = 128

spectral_scale = 8.5
beta_coef = 0.6
chem_level = 1.0
coupling = 1.0
density_floor = 0.05

PLANES = 16
WINDOWS = 8
TILES = 72
CORE = 9
QUAD = 4 * LANES
QUADS = 24
SPAN = 7


def slab_of(group, window):
    return (window // 2) * 4 + group * 2 + window % 2


def pack_kernel(
    quasi_hbm, index_hbm, mean_hbm, pairing_hbm, table_ref, out_ref,
    quasi_ref, index_ref, mean_ref, pairing_ref, rows_ref, pot_ref, sems,
):
    pairs = (
        (index_hbm, index_ref), (mean_hbm, mean_ref), (pairing_hbm, pairing_ref), (quasi_hbm, quasi_ref)
    )
    copies = [
        pltpu.make_async_copy(source, target, sems.at[k]) for k, (source, target) in enumerate(pairs)
    ]
    for copy in copies:
        copy.start()
    for window, quads in ((0, (0, 1)), (WINDOWS - 1, (SPAN - 2, SPAN - 1))):
        for group in range(2):
            for quad in quads:
                out_ref[slab_of(group, window), :, quad * QUAD : (quad + 1) * QUAD] = jnp.zeros(
                    (8, QUAD), jnp.bfloat16
                )
    copies[0].wait()
    copies[1].wait()
    index = index_ref[...]
    looked = jnp.zeros(index.shape, jnp.float32)
    for level in range(table_ref.shape[0]):
        looked = jnp.where(index == level, table_ref[level], looked)
    potential = looked + mean_ref[...]
    high = potential.astype(jnp.bfloat16).astype(jnp.float32)
    pot_ref[0] = high
    pot_ref[1] = potential - high
    for tile in range(TILES):
        lanes = slice(tile * LANES, (tile + 1) * LANES)
        for group in range(2):
            rows_ref[group, 3:4, lanes] = pot_ref[0, tile : tile + 1, :]
            rows_ref[group, 7:8, lanes] = pot_ref[1, tile : tile + 1, :]
    copies[2].wait()
    copies[3].wait()
    for group in range(2):
        for slot in range(3):
            pair = quasi_ref[3 * group + slot].astype(jnp.float32)
            rows_ref[group, slot : slot + 1, :] = pair[0:1]
            rows_ref[group, 4 + slot : 5 + slot, :] = pair[1:2]
    for quad in range(QUADS):
        first = 3 * quad
        values = jnp.concatenate(
            [pairing_ref[first : first + 3, :], jnp.zeros((1, LANES), jnp.float32)], axis=0
        )
        upper = values.astype(jnp.bfloat16).astype(jnp.float32)
        extra = jnp.concatenate([upper, values - upper], axis=0).astype(jnp.bfloat16)
        for group in range(2):
            vectors = rows_ref[group, :, first * LANES : (first + 3) * LANES].astype(jnp.bfloat16)
            for window in range(WINDOWS):
                place = quad - (3 * window - 2)
                if 0 <= place < SPAN:
                    slab, start = slab_of(group, window), place * QUAD
                    out_ref[slab, :, start : start + 3 * LANES] = vectors
                    out_ref[slab, :, start + 3 * LANES : start + QUAD] = extra


ROWS = 28
OWN = 12
STRIDE = 24
BLOCK = ROWS * STRIDE


def filter_kernel(
    msg_ref, counts_ref, slice_ref, occupation_ref, coef_ref, out_ref,
    one_ref, two_ref, a_ref, c_ref, acc_ref, density_ref,
):
    cut = lax.axis_index("cuts")
    slab = lax.axis_index("slab")
    group = (slab // 2) % 2
    window = (slab // 4) * 2 + slab % 2
    scale = 2.0 / spectral_scale
    lane = lax.broadcasted_iota(jnp.int32, (8, LANES), 1)
    below_ok = jnp.where(window > 0, 1.0, 0.0)
    above_ok = jnp.where(window < WINDOWS - 1, 1.0, 0.0)
    on_row = jnp.where(lane < NX, 1.0, 0.0).astype(jnp.float32)
    inside = [on_row * below_ok, on_row, on_row * above_ok]

    def place(y):
        return 0 if y < 8 else 1 if y < 8 + OWN else 2

    hops = [mask * (0.5 * scale) for mask in inside]

    def chosen(count, pick):
        out = lax.broadcasted_iota(jnp.int32, (count, LANES), 0)
        source = lax.broadcasted_iota(jnp.int32, (count, LANES), 1)
        same = (out % PLANES) == (source // 8)
        return jnp.where(same & pick(out // PLANES, source % 8), 1.0, 0.0).astype(jnp.bfloat16)

    gather = chosen(
        7 * PLANES,
        lambda i, row: (row == (i // 3) * 4 + i % 3) | ((i == 6) & (row % 4 == 3)),
    )
    spread = chosen(3 * PLANES, lambda part, row: row % 4 == part)

    for ref in (one_ref, two_ref):
        for block in range(6 * ROWS + 1):
            ref[block * STRIDE : block * STRIDE + 8, :] = jnp.zeros((8, LANES), jnp.float32)
    density_ref[...] = jnp.zeros_like(density_ref)

    def unpack(tiles):
        first, second, third = tiles
        wide = lax.broadcasted_iota(jnp.int32, first.shape, 1)
        ok = wide < NX
        rows = [
            first,
            jnp.where(wide < 32, pltpu.roll(first, 32, 1), pltpu.roll(second, 32, 1)),
            jnp.where(wide < 64, pltpu.roll(second, 64, 1), pltpu.roll(third, 64, 1)),
            pltpu.roll(third, 96, 1),
        ]
        return [jnp.where(ok, row, 0.0) for row in rows]

    for quad in range(ROWS // 4):
        start = quad * QUAD
        taken = jnp.dot(
            gather, msg_ref[:, start : start + 3 * LANES], preferred_element_type=jnp.float32
        )
        part = jnp.dot(
            spread, msg_ref[:, start + 3 * LANES : start + QUAD], preferred_element_type=jnp.float32
        )
        rows = unpack([taken[:, k * LANES : (k + 1) * LANES] for k in range(3)])
        pairs = unpack([part[16 * k : 16 * k + 16] for k in range(3)])
        for k in range(4):
            y = 4 * quad + k
            mask = inside[place(y)]
            for i in range(6):
                base = i * BLOCK + y * STRIDE + 8
                one_ref[base : base + 16, :] = rows[k][16 * i : 16 * i + 16]
            for high in range(2):
                at = slice(16 * y + 8 * high, 16 * y + 8 * high + 8)
                a_ref[at, :] = (rows[k][96 + 8 * high : 104 + 8 * high] + 3.0) * (mask * scale)
                c_ref[at, :] = pairs[k][8 * high : 8 * high + 8] * (mask * scale)

    live = counts_ref[cut]
    start = cut * CAP + group * 3

    def vector(slot, carry):
        which = slice_ref[start + slot]
        weight = jnp.where(group * 3 + slot < live, occupation_ref[start + slot], 0.0)
        coefs = [coef_ref[which, order] for order in range(DEGREE + 1)]
        shift = slot * BLOCK

        def load(ref, comp, y, offset):
            origin = pl.multiple_of(shift + comp * 3 * BLOCK, 8)
            return ref[pl.ds(origin + y * STRIDE + 8 + offset, 8), :]

        for order in range(1, DEGREE + 1):
            now, other = (one_ref, two_ref) if order % 2 == 1 else (two_ref, one_ref)
            for y in range(order, ROWS - order):
                hop = hops[place(y)]
                for high in range(2):
                    z = 8 * high
                    onsite = a_ref[16 * y + z : 16 * y + z + 8, :]
                    cross = c_ref[16 * y + z : 16 * y + z + 8, :]
                    middles, singles = [], []
                    for comp in range(2):
                        middle = load(now, comp, y, z)
                        beside = pltpu.roll(middle, 1, 1) + pltpu.roll(middle, LANES - 1, 1)
                        beside = beside + (load(now, comp, y - 1, z) + load(now, comp, y + 1, z))
                        beside = beside + (load(now, comp, y, z - 1) + load(now, comp, y, z + 1))
                        middles.append(middle)
                        singles.append(onsite * middle - hop * beside)
                    results = [
                        singles[0] + cross * middles[1],
                        cross * middles[0] - singles[1],
                    ]
                    totals = []
                    for comp in range(2):
                        result = results[comp]
                        if order == 1:
                            result = 0.5 * result
                        else:
                            result = result - load(other, comp, y, z)
                        if order < DEGREE:
                            origin = pl.multiple_of(shift + comp * 3 * BLOCK, 8)
                            other[pl.ds(origin + y * STRIDE + 8 + z, 8), :] = result
                        if 8 <= y < 8 + OWN:
                            at = (comp * OWN + y - 8) * 16 + z
                            if order == 1:
                                total = coefs[0] * middles[comp] + coefs[1] * result
                            else:
                                total = acc_ref[at : at + 8, :] + coefs[order] * result
                            if order < DEGREE:
                                acc_ref[at : at + 8, :] = total
                            totals.append(total)
                    if order == DEGREE:
                        weighted = weight * totals[1]
                        at = (y - 8) * 16 + z
                        density_ref[at : at + 8, :] += weighted * totals[1]
                        at = at + OWN * 16
                        density_ref[at : at + 8, :] += weighted * totals[0]
        return carry

    lax.fori_loop(0, 3, vector, 0)

    for quarter in range(4):
        for high in range(2):
            at = 48 * quarter + 8 * high
            normal = [density_ref[at + 16 * k : at + 16 * k + 8, :] for k in range(3)]
            at = at + OWN * 16
            other = [density_ref[at + 16 * k : at + 16 * k + 8, :] for k in range(3)]
            second, third = pltpu.roll(normal[1], 96, 1), pltpu.roll(normal[2], 64, 1)
            last = pltpu.roll(other[2], 96, 1)
            tiles = [
                jnp.where(lane < 96, normal[0], second),
                jnp.where(lane < 64, second, third),
                jnp.where(lane < 32, third, pltpu.roll(other[0], 32, 1)),
                jnp.where(lane < 96, other[1], last),
                last[:, :64],
            ]
            for k in range(8):
                piece = piece_of(8 * high + k, quarter)
                for tile, values in enumerate(tiles):
                    lanes = slice(tile * LANES, tile * LANES + values.shape[1])
                    out_ref[piece, :, lanes] = values[k : k + 1]


def piece_of(plane, quarter):
    cut = 4 * (2 * (plane // 4) + plane % 2) + quarter
    return 2 * cut + (plane // 2) % 2


def sum_kernel(parts_ref, out_ref):
    out_ref[...] = jnp.sum(parts_ref[...], axis=0)


def vmem(count):
    return [pl.BlockSpec(memory_space=pltpu.VMEM)] * count


def smem(count):
    return [pl.BlockSpec(memory_space=pltpu.SMEM)] * count


def grant(mebibytes):
    return pltpu.CompilerParams(vmem_limit_bytes=mebibytes << 20)


def filter_call(message, counts, slot_slice, occupation, filter_coef):
    return pl.pallas_call(
        filter_kernel,
        out_shape=jax.ShapeDtypeStruct((64, 1, 2 * 288), jnp.float32),
        in_specs=vmem(1) + smem(4),
        out_specs=pl.BlockSpec(memory_space=pltpu.VMEM),
        scratch_shapes=[
            pltpu.VMEM((6 * BLOCK + 8, LANES), jnp.float32),
            pltpu.VMEM((6 * BLOCK + 8, LANES), jnp.float32),
            pltpu.VMEM((16 * ROWS, LANES), jnp.float32),
            pltpu.VMEM((16 * ROWS, LANES), jnp.float32),
            pltpu.VMEM((2 * OWN * 16, LANES), jnp.float32),
            pltpu.VMEM((2 * OWN * 16, LANES), jnp.float32),
        ],
        compiler_params=grant(16),
        name="filter",
    )(message.reshape(8 * PLANES, SPAN * QUAD), counts, slot_slice, occupation, filter_coef)


def summing_groups():
    return [
        [cut * 16 + slab_of(group, window) for cut in range(32) for group in range(2)]
        for window in range(WINDOWS)
    ]


def routes():
    pairs = []
    for window in range(WINDOWS):
        for plane in range(PLANES):
            for quarter in range(4):
                piece = piece_of(plane, quarter)
                source = (piece // 2) * 16 + slab_of(piece % 2, window)
                pairs.append((source, (4 * window + quarter) * 16 + plane))
    return pairs


def body(
    quasi, counts, slot_slice, occupation, filter_coef, trap_index, trap_table, mean_field, pairing
):
    share = mean_field.shape[1] // lax.axis_size("cuts")
    packed = jnp.transpose(quasi, (1, 2, 0, 3)).reshape(CAP, 2, TILES * LANES)
    message = pl.pallas_call(
        pack_kernel,
        out_shape=jax.ShapeDtypeStruct((PLANES, 8, SPAN * QUAD), jnp.bfloat16),
        in_specs=[pl.BlockSpec(memory_space=pltpu.HBM)] * 4 + smem(1),
        out_specs=pl.BlockSpec(memory_space=pltpu.VMEM),
        scratch_shapes=[
            pltpu.VMEM((CAP, 2, TILES * LANES), jnp.bfloat16),
            pltpu.VMEM((TILES, LANES), jnp.int32),
            pltpu.VMEM((TILES, LANES), jnp.float32),
            pltpu.VMEM((TILES, LANES), jnp.float32),
            pltpu.VMEM((2, 8, TILES * LANES), jnp.float32),
            pltpu.VMEM((2, TILES, LANES), jnp.float32),
            pltpu.SemaphoreType.DMA((4,)),
        ],
        name="pack",
    )(
        packed,
        trap_index.reshape(TILES, LANES),
        mean_field.reshape(TILES, LANES),
        pairing.reshape(TILES, LANES),
        trap_table,
    )
    message = lax.all_to_all(message, "slab", 0, 0, tiled=True)
    parts = filter_call(message, counts, slot_slice, occupation, filter_coef)
    parts = lax.all_to_all(
        parts, ("cuts", "slab"), 0, 0, axis_index_groups=summing_groups(), tiled=True
    )
    sums = pl.pallas_call(
        sum_kernel,
        out_shape=jax.ShapeDtypeStruct((1, 2 * 288), jnp.float32),
        in_specs=vmem(1),
        out_specs=pl.BlockSpec(memory_space=pltpu.VMEM),
        compiler_params=grant(4),
        name="total",
    )(parts)
    sums = lax.ppermute(sums, ("cuts", "slab"), routes())
    offset = lax.axis_index("cuts") * share
    mean_local = lax.dynamic_slice_in_dim(mean_field, offset, share, 1)
    pairing_local = lax.dynamic_slice_in_dim(pairing, offset, share, 1)
    normal_density = sums[:, :share]
    anomalous_density = sums[:, share:]
    cube_root = jnp.cbrt(normal_density + density_floor)
    new_mean_field = 0.5 * mean_local + 0.5 * (beta_coef * cube_root * cube_root - chem_level)
    new_pairing = 0.5 * pairing_local - coupling * anomalous_density
    return (normal_density, anomalous_density, new_mean_field, new_pairing)


def solution(mesh):
    return jax.shard_map(
        body,
        mesh=mesh,
        in_specs=(
            P(None, "cuts", "slab", None),
            P(),
            P(),
            P(),
            P(),
            P("slab", None),
            P(),
            P("slab", None),
            P("slab", None),
        ),
        out_specs=(P("slab", "cuts"), P("slab", "cuts"), P("slab", "cuts"), P("slab", "cuts")),
        check_vma=False,
    )
```

```python
import jax
import jax.numpy as jnp
from jax import lax
from jax.experimental import pallas as pl
from jax.experimental.pallas import tpu as pltpu
from jax.sharding import PartitionSpec as P

NX = 96
DEGREE = 8
CAP = 6
LANES = 128

spectral_scale = 8.5
beta_coef = 0.6
chem_level = 1.0
coupling = 1.0
density_floor = 0.05

PLANES = 16
WINDOWS = 8
TILES = 72
CORE = 9
QUAD = 4 * LANES
MESSAGE = 3 * QUAD
HALO = 2 * QUAD


def slab_of(group, window):
    return (window // 2) * 4 + group * 2 + window % 2


def pack_kernel(quasi_ref, index_ref, mean_ref, pairing_ref, table_ref, out_ref, rows_ref, pot_ref):
    index = index_ref[...]
    looked = jnp.zeros(index.shape, jnp.float32)
    for level in range(table_ref.shape[0]):
        looked = jnp.where(index == level, table_ref[level], looked)
    potential = looked + mean_ref[...]
    high = potential.astype(jnp.bfloat16).astype(jnp.float32)
    pot_ref[0] = high
    pot_ref[1] = potential - high
    for group in range(2):
        for slot in range(3):
            pair = quasi_ref[3 * group + slot].astype(jnp.float32)
            rows_ref[group, slot : slot + 1, :] = pair[0:1]
            rows_ref[group, 4 + slot : 5 + slot, :] = pair[1:2]
        for tile in range(TILES):
            lanes = slice(tile * LANES, (tile + 1) * LANES)
            rows_ref[group, 3:4, lanes] = pot_ref[0, tile : tile + 1, :]
            rows_ref[group, 7:8, lanes] = pot_ref[1, tile : tile + 1, :]
    for window in range(WINDOWS):
        for quad in range(3):
            first = CORE * window + 3 * quad
            values = jnp.concatenate(
                [pairing_ref[first : first + 3, :], jnp.zeros((1, LANES), jnp.float32)], axis=0
            )
            upper = values.astype(jnp.bfloat16).astype(jnp.float32)
            extra = jnp.concatenate([upper, values - upper], axis=0).astype(jnp.bfloat16)
            start = quad * QUAD
            for group in range(2):
                slab = slab_of(group, window)
                out_ref[slab, :, start : start + 3 * LANES] = rows_ref[
                    group, :, first * LANES : (first + 3) * LANES
                ].astype(jnp.bfloat16)
                out_ref[slab, :, start + 3 * LANES : start + QUAD] = extra


ROWS = 28
OWN = 12
STRIDE = 24
BLOCK = ROWS * STRIDE


def filter_kernel(
    low_ref, own_ref, high_ref, counts_ref, slice_ref, occupation_ref, coef_ref, out_ref,
    one_ref, two_ref, a_ref, c_ref, acc_ref, density_ref,
):
    cut = lax.axis_index("cuts")
    slab = lax.axis_index("slab")
    group = (slab // 2) % 2
    window = (slab // 4) * 2 + slab % 2
    scale = 2.0 / spectral_scale
    lane = lax.broadcasted_iota(jnp.int32, (8, LANES), 1)
    below_ok = jnp.where(window > 0, 1.0, 0.0)
    above_ok = jnp.where(window < WINDOWS - 1, 1.0, 0.0)
    on_row = jnp.where(lane < NX, 1.0, 0.0).astype(jnp.float32)
    inside = [on_row * below_ok, on_row, on_row * above_ok]

    def place(y):
        return 0 if y < 8 else 1 if y < 8 + OWN else 2

    hops = [mask * (0.5 * scale) for mask in inside]

    def chosen(count, pick):
        out = lax.broadcasted_iota(jnp.int32, (count, LANES), 0)
        source = lax.broadcasted_iota(jnp.int32, (count, LANES), 1)
        same = (out % PLANES) == (source // 8)
        return jnp.where(same & pick(out // PLANES, source % 8), 1.0, 0.0).astype(jnp.bfloat16)

    gather = chosen(
        7 * PLANES,
        lambda i, row: (row == (i // 3) * 4 + i % 3) | ((i == 6) & (row % 4 == 3)),
    )
    spread = chosen(3 * PLANES, lambda part, row: row % 4 == part)

    for ref in (one_ref, two_ref):
        for block in range(6 * ROWS + 1):
            ref[block * STRIDE : block * STRIDE + 8, :] = jnp.zeros((8, LANES), jnp.float32)
    density_ref[...] = jnp.zeros_like(density_ref)

    def unpack(tiles):
        first, second, third = tiles
        wide = lax.broadcasted_iota(jnp.int32, first.shape, 1)
        ok = wide < NX
        rows = [
            first,
            jnp.where(wide < 32, pltpu.roll(first, 32, 1), pltpu.roll(second, 32, 1)),
            jnp.where(wide < 64, pltpu.roll(second, 64, 1), pltpu.roll(third, 64, 1)),
            pltpu.roll(third, 96, 1),
        ]
        return [jnp.where(ok, row, 0.0) for row in rows]

    for quad in range(ROWS // 4):
        if quad < 2:
            ref, start = low_ref, quad * QUAD
        elif quad < 5:
            ref, start = own_ref, (quad - 2) * QUAD
        else:
            ref, start = high_ref, (quad - 5) * QUAD
        taken = jnp.dot(
            gather, ref[:, start : start + 3 * LANES], preferred_element_type=jnp.float32
        )
        part = jnp.dot(
            spread, ref[:, start + 3 * LANES : start + QUAD], preferred_element_type=jnp.float32
        )
        rows = unpack([taken[:, k * LANES : (k + 1) * LANES] for k in range(3)])
        pairs = unpack([part[16 * k : 16 * k + 16] for k in range(3)])
        for k in range(4):
            y = 4 * quad + k
            mask = inside[place(y)]
            for i in range(6):
                base = i * BLOCK + y * STRIDE + 8
                one_ref[base : base + 16, :] = rows[k][16 * i : 16 * i + 16]
            for high in range(2):
                at = slice(16 * y + 8 * high, 16 * y + 8 * high + 8)
                a_ref[at, :] = (rows[k][96 + 8 * high : 104 + 8 * high] + 3.0) * (mask * scale)
                c_ref[at, :] = pairs[k][8 * high : 8 * high + 8] * (mask * scale)

    live = counts_ref[cut]
    start = cut * CAP + group * 3

    def vector(slot, carry):
        which = slice_ref[start + slot]
        weight = jnp.where(group * 3 + slot < live, occupation_ref[start + slot], 0.0)
        coefs = [coef_ref[which, order] for order in range(DEGREE + 1)]
        shift = slot * BLOCK

        def load(ref, comp, y, offset):
            origin = pl.multiple_of(shift + comp * 3 * BLOCK, 8)
            return ref[pl.ds(origin + y * STRIDE + 8 + offset, 8), :]

        for order in range(1, DEGREE + 1):
            now, other = (one_ref, two_ref) if order % 2 == 1 else (two_ref, one_ref)
            for y in range(order, ROWS - order):
                hop = hops[place(y)]
                for high in range(2):
                    z = 8 * high
                    onsite = a_ref[16 * y + z : 16 * y + z + 8, :]
                    cross = c_ref[16 * y + z : 16 * y + z + 8, :]
                    middles, singles = [], []
                    for comp in range(2):
                        middle = load(now, comp, y, z)
                        beside = pltpu.roll(middle, 1, 1) + pltpu.roll(middle, LANES - 1, 1)
                        beside = beside + (load(now, comp, y - 1, z) + load(now, comp, y + 1, z))
                        beside = beside + (load(now, comp, y, z - 1) + load(now, comp, y, z + 1))
                        middles.append(middle)
                        singles.append(onsite * middle - hop * beside)
                    results = [
                        singles[0] + cross * middles[1],
                        cross * middles[0] - singles[1],
                    ]
                    totals = []
                    for comp in range(2):
                        result = results[comp]
                        if order == 1:
                            result = 0.5 * result
                        else:
                            result = result - load(other, comp, y, z)
                        if order < DEGREE:
                            origin = pl.multiple_of(shift + comp * 3 * BLOCK, 8)
                            other[pl.ds(origin + y * STRIDE + 8 + z, 8), :] = result
                        if 8 <= y < 8 + OWN:
                            at = (comp * OWN + y - 8) * 16 + z
                            if order == 1:
                                total = coefs[0] * middles[comp] + coefs[1] * result
                            else:
                                total = acc_ref[at : at + 8, :] + coefs[order] * result
                            if order < DEGREE:
                                acc_ref[at : at + 8, :] = total
                            totals.append(total)
                    if order == DEGREE:
                        weighted = weight * totals[1]
                        at = (y - 8) * 16 + z
                        density_ref[at : at + 8, :] += weighted * totals[1]
                        at = at + OWN * 16
                        density_ref[at : at + 8, :] += weighted * totals[0]
        return carry

    lax.fori_loop(0, 3, vector, 0)

    for quarter in range(4):
        for high in range(2):
            at = 48 * quarter + 8 * high
            normal = [density_ref[at + 16 * k : at + 16 * k + 8, :] for k in range(3)]
            at = at + OWN * 16
            other = [density_ref[at + 16 * k : at + 16 * k + 8, :] for k in range(3)]
            second, third = pltpu.roll(normal[1], 96, 1), pltpu.roll(normal[2], 64, 1)
            last = pltpu.roll(other[2], 96, 1)
            tiles = [
                jnp.where(lane < 96, normal[0], second),
                jnp.where(lane < 64, second, third),
                jnp.where(lane < 32, third, pltpu.roll(other[0], 32, 1)),
                jnp.where(lane < 96, other[1], last),
                last[:, :64],
            ]
            for k in range(8):
                piece = piece_of(8 * high + k, quarter)
                for tile, values in enumerate(tiles):
                    lanes = slice(tile * LANES, tile * LANES + values.shape[1])
                    out_ref[piece, :, lanes] = values[k : k + 1]


def piece_of(plane, quarter):
    cut = 4 * (2 * (plane // 4) + plane % 2) + quarter
    return 2 * cut + (plane // 2) % 2


def sum_kernel(parts_ref, out_ref):
    out_ref[...] = jnp.sum(parts_ref[...], axis=0)


def vmem(count):
    return [pl.BlockSpec(memory_space=pltpu.VMEM)] * count


def smem(count):
    return [pl.BlockSpec(memory_space=pltpu.SMEM)] * count


def grant(mebibytes):
    return pltpu.CompilerParams(vmem_limit_bytes=mebibytes << 20)


def filter_call(low, own, high, counts, slot_slice, occupation, filter_coef):
    flat = [part.reshape(8 * PLANES, part.shape[2]) for part in (low, own, high)]
    return pl.pallas_call(
        filter_kernel,
        out_shape=jax.ShapeDtypeStruct((64, 1, 2 * 288), jnp.float32),
        in_specs=vmem(3) + smem(4),
        out_specs=pl.BlockSpec(memory_space=pltpu.VMEM),
        scratch_shapes=[
            pltpu.VMEM((6 * BLOCK + 8, LANES), jnp.float32),
            pltpu.VMEM((6 * BLOCK + 8, LANES), jnp.float32),
            pltpu.VMEM((16 * ROWS, LANES), jnp.float32),
            pltpu.VMEM((16 * ROWS, LANES), jnp.float32),
            pltpu.VMEM((2 * OWN * 16, LANES), jnp.float32),
            pltpu.VMEM((2 * OWN * 16, LANES), jnp.float32),
        ],
        compiler_params=grant(16),
        name="filter",
    )(*flat, counts, slot_slice, occupation, filter_coef)


def neighbours(by):
    return [
        (slab_of(group, window), slab_of(group, window + by))
        for group in range(2)
        for window in range(WINDOWS)
        if 0 <= window + by < WINDOWS
    ]


def summing_groups():
    return [
        [cut * 16 + slab_of(group, window) for cut in range(32) for group in range(2)]
        for window in range(WINDOWS)
    ]


def routes():
    pairs = []
    for window in range(WINDOWS):
        for plane in range(PLANES):
            for quarter in range(4):
                piece = piece_of(plane, quarter)
                source = (piece // 2) * 16 + slab_of(piece % 2, window)
                pairs.append((source, (4 * window + quarter) * 16 + plane))
    return pairs


def body(
    quasi, counts, slot_slice, occupation, filter_coef, trap_index, trap_table, mean_field, pairing
):
    share = mean_field.shape[1] // lax.axis_size("cuts")
    packed = jnp.transpose(quasi, (1, 2, 0, 3)).reshape(CAP, 2, TILES * LANES)
    message = pl.pallas_call(
        pack_kernel,
        out_shape=jax.ShapeDtypeStruct((PLANES, 8, MESSAGE), jnp.bfloat16),
        in_specs=vmem(4) + smem(1),
        out_specs=pl.BlockSpec(memory_space=pltpu.VMEM),
        scratch_shapes=[
            pltpu.VMEM((2, 8, TILES * LANES), jnp.float32),
            pltpu.VMEM((2, TILES, LANES), jnp.float32),
        ],
        name="pack",
    )(
        packed,
        trap_index.reshape(TILES, LANES),
        mean_field.reshape(TILES, LANES),
        pairing.reshape(TILES, LANES),
        trap_table,
    )
    message = lax.all_to_all(message, "slab", 0, 0, tiled=True)
    low = lax.ppermute(message[:, :, MESSAGE - HALO :], "slab", neighbours(1))
    high = lax.ppermute(message[:, :, :HALO], "slab", neighbours(-1))
    parts = filter_call(low, message, high, counts, slot_slice, occupation, filter_coef)
    parts = lax.all_to_all(
        parts, ("cuts", "slab"), 0, 0, axis_index_groups=summing_groups(), tiled=True
    )
    sums = pl.pallas_call(
        sum_kernel,
        out_shape=jax.ShapeDtypeStruct((1, 2 * 288), jnp.float32),
        in_specs=vmem(1),
        out_specs=pl.BlockSpec(memory_space=pltpu.VMEM),
        compiler_params=grant(4),
        name="total",
    )(parts)
    sums = lax.ppermute(sums, ("cuts", "slab"), routes())
    offset = lax.axis_index("cuts") * share
    mean_local = lax.dynamic_slice_in_dim(mean_field, offset, share, 1)
    pairing_local = lax.dynamic_slice_in_dim(pairing, offset, share, 1)
    normal_density = sums[:, :share]
    anomalous_density = sums[:, share:]
    cube_root = jnp.cbrt(normal_density + density_floor)
    new_mean_field = 0.5 * mean_local + 0.5 * (beta_coef * cube_root * cube_root - chem_level)
    new_pairing = 0.5 * pairing_local - coupling * anomalous_density
    return (normal_density, anomalous_density, new_mean_field, new_pairing)


def solution(mesh):
    return jax.shard_map(
        body,
        mesh=mesh,
        in_specs=(
            P(None, "cuts", "slab", None),
            P(),
            P(),
            P(),
            P(),
            P("slab", None),
            P(),
            P("slab", None),
            P("slab", None),
        ),
        out_specs=(P("slab", "cuts"), P("slab", "cuts"), P("slab", "cuts"), P("slab", "cuts")),
        check_vma=False,
    )
```

```python
import jax
import jax.numpy as jnp
from jax import lax
from jax.experimental import pallas as pl
from jax.experimental.pallas import tpu as pltpu
from jax.sharding import PartitionSpec as P

NX = 96
DEGREE = 8
CAP = 6
LANES = 128

spectral_scale = 8.5
beta_coef = 0.6
chem_level = 1.0
coupling = 1.0
density_floor = 0.05

PLANES = 16
WINDOWS = 8
TILES = 72
CORE = 9
QUAD = 4 * LANES
MESSAGE = 3 * QUAD
HALO = 2 * QUAD


def slab_of(group, window):
    return (window // 2) * 4 + group * 2 + window % 2


def pack_kernel(
    quasi_hbm, index_hbm, mean_hbm, pairing_hbm, table_ref, counts_ref, slice_ref, occupation_ref, coef_ref,
    out_ref, terms_ref,
    quasi_ref, index_ref, mean_ref, pairing_ref, rows_ref, pot_ref, sems,
):
    pairs = (
        (index_hbm, index_ref), (mean_hbm, mean_ref), (pairing_hbm, pairing_ref), (quasi_hbm, quasi_ref)
    )
    copies = [
        pltpu.make_async_copy(source, target, sems.at[k]) for k, (source, target) in enumerate(pairs)
    ]
    for copy in copies:
        copy.start()
    cut = lax.axis_index("cuts")
    half = (lax.axis_index("slab") // 2) % 2
    live = counts_ref[cut]
    for slot in range(3):
        place = half * 3 + slot
        which = slice_ref[cut * CAP + place]
        for order in range(DEGREE + 1):
            terms_ref[16 * slot + order] = coef_ref[which, order]
        terms_ref[16 * slot + 9] = jnp.where(place < live, occupation_ref[cut * CAP + place], 0.0)
    for copy in copies:
        copy.wait()
    index = index_ref[...]
    looked = jnp.zeros(index.shape, jnp.float32)
    for level in range(table_ref.shape[0]):
        looked = jnp.where(index == level, table_ref[level], looked)
    potential = looked + mean_ref[...]
    high = potential.astype(jnp.bfloat16).astype(jnp.float32)
    pot_ref[0] = high
    pot_ref[1] = potential - high
    for group in range(2):
        for slot in range(3):
            pair = quasi_ref[3 * group + slot].astype(jnp.float32)
            rows_ref[group, slot : slot + 1, :] = pair[0:1]
            rows_ref[group, 4 + slot : 5 + slot, :] = pair[1:2]
        for tile in range(TILES):
            lanes = slice(tile * LANES, (tile + 1) * LANES)
            rows_ref[group, 3:4, lanes] = pot_ref[0, tile : tile + 1, :]
            rows_ref[group, 7:8, lanes] = pot_ref[1, tile : tile + 1, :]
    for window in range(WINDOWS):
        for quad in range(3):
            first = CORE * window + 3 * quad
            values = jnp.concatenate(
                [pairing_ref[first : first + 3, :], jnp.zeros((1, LANES), jnp.float32)], axis=0
            )
            upper = values.astype(jnp.bfloat16).astype(jnp.float32)
            extra = jnp.concatenate([upper, values - upper], axis=0).astype(jnp.bfloat16)
            start = quad * QUAD
            for group in range(2):
                slab = slab_of(group, window)
                out_ref[slab, :, start : start + 3 * LANES] = rows_ref[
                    group, :, first * LANES : (first + 3) * LANES
                ].astype(jnp.bfloat16)
                out_ref[slab, :, start + 3 * LANES : start + QUAD] = extra


ROWS = 28
OWN = 12
STRIDE = 24
BLOCK = ROWS * STRIDE


def filter_kernel(
    low_ref, own_ref, high_ref, terms_ref, out_ref,
    one_ref, two_ref, a_ref, c_ref, acc_ref, density_ref,
):
    slab = lax.axis_index("slab")
    window = (slab // 4) * 2 + slab % 2
    scale = 2.0 / spectral_scale
    lane = lax.broadcasted_iota(jnp.int32, (8, LANES), 1)
    below_ok = jnp.where(window > 0, 1.0, 0.0)
    above_ok = jnp.where(window < WINDOWS - 1, 1.0, 0.0)
    on_row = jnp.where(lane < NX, 1.0, 0.0).astype(jnp.float32)
    inside = [on_row * below_ok, on_row, on_row * above_ok]

    def place(y):
        return 0 if y < 8 else 1 if y < 8 + OWN else 2

    hops = [mask * (0.5 * scale) for mask in inside]

    def chosen(count, pick):
        out = lax.broadcasted_iota(jnp.int32, (count, LANES), 0)
        source = lax.broadcasted_iota(jnp.int32, (count, LANES), 1)
        same = (out % PLANES) == (source // 8)
        return jnp.where(same & pick(out // PLANES, source % 8), 1.0, 0.0).astype(jnp.bfloat16)

    gather = chosen(
        7 * PLANES,
        lambda i, row: (row == (i // 3) * 4 + i % 3) | ((i == 6) & (row % 4 == 3)),
    )
    spread = chosen(3 * PLANES, lambda part, row: row % 4 == part)

    for ref in (one_ref, two_ref):
        for block in range(6 * ROWS + 1):
            ref[block * STRIDE : block * STRIDE + 8, :] = jnp.zeros((8, LANES), jnp.float32)
    density_ref[...] = jnp.zeros_like(density_ref)

    def unpack(tiles):
        first, second, third = tiles
        wide = lax.broadcasted_iota(jnp.int32, first.shape, 1)
        ok = wide < NX
        rows = [
            first,
            jnp.where(wide < 32, pltpu.roll(first, 32, 1), pltpu.roll(second, 32, 1)),
            jnp.where(wide < 64, pltpu.roll(second, 64, 1), pltpu.roll(third, 64, 1)),
            pltpu.roll(third, 96, 1),
        ]
        return [jnp.where(ok, row, 0.0) for row in rows]

    for quad in range(ROWS // 4):
        if quad < 2:
            ref, start = low_ref, quad * QUAD
        elif quad < 5:
            ref, start = own_ref, (quad - 2) * QUAD
        else:
            ref, start = high_ref, (quad - 5) * QUAD
        taken = jnp.dot(
            gather, ref[:, start : start + 3 * LANES], preferred_element_type=jnp.float32
        )
        part = jnp.dot(
            spread, ref[:, start + 3 * LANES : start + QUAD], preferred_element_type=jnp.float32
        )
        rows = unpack([taken[:, k * LANES : (k + 1) * LANES] for k in range(3)])
        pairs = unpack([part[16 * k : 16 * k + 16] for k in range(3)])
        for k in range(4):
            y = 4 * quad + k
            mask = inside[place(y)]
            for i in range(6):
                base = i * BLOCK + y * STRIDE + 8
                one_ref[base : base + 16, :] = rows[k][16 * i : 16 * i + 16]
            for high in range(2):
                at = slice(16 * y + 8 * high, 16 * y + 8 * high + 8)
                a_ref[at, :] = (rows[k][96 + 8 * high : 104 + 8 * high] + 3.0) * (mask * scale)
                c_ref[at, :] = pairs[k][8 * high : 8 * high + 8] * (mask * scale)

    def vector(slot, carry):
        coefs = [terms_ref[16 * slot + order] for order in range(DEGREE + 1)]
        weight = terms_ref[16 * slot + 9]
        shift = slot * BLOCK

        def load(ref, comp, y, offset):
            origin = pl.multiple_of(shift + comp * 3 * BLOCK, 8)
            return ref[pl.ds(origin + y * STRIDE + 8 + offset, 8), :]

        for order in range(1, DEGREE + 1):
            now, other = (one_ref, two_ref) if order % 2 == 1 else (two_ref, one_ref)
            for y in range(order, ROWS - order):
                hop = hops[place(y)]
                for high in range(2):
                    z = 8 * high
                    onsite = a_ref[16 * y + z : 16 * y + z + 8, :]
                    cross = c_ref[16 * y + z : 16 * y + z + 8, :]
                    middles, singles = [], []
                    for comp in range(2):
                        middle = load(now, comp, y, z)
                        beside = pltpu.roll(middle, 1, 1) + pltpu.roll(middle, LANES - 1, 1)
                        beside = beside + (load(now, comp, y - 1, z) + load(now, comp, y + 1, z))
                        beside = beside + (load(now, comp, y, z - 1) + load(now, comp, y, z + 1))
                        middles.append(middle)
                        singles.append(onsite * middle - hop * beside)
                    results = [
                        singles[0] + cross * middles[1],
                        cross * middles[0] - singles[1],
                    ]
                    totals = []
                    for comp in range(2):
                        result = results[comp]
                        if order == 1:
                            result = 0.5 * result
                        else:
                            result = result - load(other, comp, y, z)
                        if order < DEGREE:
                            origin = pl.multiple_of(shift + comp * 3 * BLOCK, 8)
                            other[pl.ds(origin + y * STRIDE + 8 + z, 8), :] = result
                        if 8 <= y < 8 + OWN:
                            at = (comp * OWN + y - 8) * 16 + z
                            if order == 1:
                                total = coefs[0] * middles[comp] + coefs[1] * result
                            else:
                                total = acc_ref[at : at + 8, :] + coefs[order] * result
                            if order < DEGREE:
                                acc_ref[at : at + 8, :] = total
                            totals.append(total)
                    if order == DEGREE:
                        weighted = weight * totals[1]
                        at = (y - 8) * 16 + z
                        density_ref[at : at + 8, :] += weighted * totals[1]
                        at = at + OWN * 16
                        density_ref[at : at + 8, :] += weighted * totals[0]
        return carry

    lax.fori_loop(0, 3, vector, 0)

    for quarter in range(4):
        for high in range(2):
            at = 48 * quarter + 8 * high
            normal = [density_ref[at + 16 * k : at + 16 * k + 8, :] for k in range(3)]
            at = at + OWN * 16
            other = [density_ref[at + 16 * k : at + 16 * k + 8, :] for k in range(3)]
            second, third = pltpu.roll(normal[1], 96, 1), pltpu.roll(normal[2], 64, 1)
            last = pltpu.roll(other[2], 96, 1)
            tiles = [
                jnp.where(lane < 96, normal[0], second),
                jnp.where(lane < 64, second, third),
                jnp.where(lane < 32, third, pltpu.roll(other[0], 32, 1)),
                jnp.where(lane < 96, other[1], last),
                last[:, :64],
            ]
            for k in range(8):
                piece = piece_of(8 * high + k, quarter)
                for tile, values in enumerate(tiles):
                    lanes = slice(tile * LANES, tile * LANES + values.shape[1])
                    out_ref[piece, :, lanes] = values[k : k + 1]


def piece_of(plane, quarter):
    cut = 4 * (2 * (plane // 4) + plane % 2) + quarter
    return 2 * cut + (plane // 2) % 2


def sum_kernel(parts_ref, out_ref):
    out_ref[...] = jnp.sum(parts_ref[...], axis=0)


def vmem(count):
    return [pl.BlockSpec(memory_space=pltpu.VMEM)] * count


def smem(count):
    return [pl.BlockSpec(memory_space=pltpu.SMEM)] * count


def grant(mebibytes):
    return pltpu.CompilerParams(vmem_limit_bytes=mebibytes << 20)


def filter_call(low, own, high, terms):
    flat = [part.reshape(8 * PLANES, part.shape[2]) for part in (low, own, high)]
    return pl.pallas_call(
        filter_kernel,
        out_shape=jax.ShapeDtypeStruct((64, 1, 2 * 288), jnp.float32),
        in_specs=vmem(3) + smem(1),
        out_specs=pl.BlockSpec(memory_space=pltpu.VMEM),
        scratch_shapes=[
            pltpu.VMEM((6 * BLOCK + 8, LANES), jnp.float32),
            pltpu.VMEM((6 * BLOCK + 8, LANES), jnp.float32),
            pltpu.VMEM((16 * ROWS, LANES), jnp.float32),
            pltpu.VMEM((16 * ROWS, LANES), jnp.float32),
            pltpu.VMEM((2 * OWN * 16, LANES), jnp.float32),
            pltpu.VMEM((2 * OWN * 16, LANES), jnp.float32),
        ],
        compiler_params=grant(16),
        name="filter",
    )(*flat, terms)


def neighbours(by):
    return [
        (slab_of(group, window), slab_of(group, window + by))
        for group in range(2)
        for window in range(WINDOWS)
        if 0 <= window + by < WINDOWS
    ]


def summing_groups():
    return [
        [cut * 16 + slab_of(group, window) for cut in range(32) for group in range(2)]
        for window in range(WINDOWS)
    ]


def routes():
    pairs = []
    for window in range(WINDOWS):
        for plane in range(PLANES):
            for quarter in range(4):
                piece = piece_of(plane, quarter)
                source = (piece // 2) * 16 + slab_of(piece % 2, window)
                pairs.append((source, (4 * window + quarter) * 16 + plane))
    return pairs


def body(
    quasi, counts, slot_slice, occupation, filter_coef, trap_index, trap_table, mean_field, pairing
):
    share = mean_field.shape[1] // lax.axis_size("cuts")
    packed = jnp.transpose(quasi, (1, 2, 0, 3)).reshape(CAP, 2, TILES * LANES)
    message, terms = pl.pallas_call(
        pack_kernel,
        out_shape=[
            jax.ShapeDtypeStruct((PLANES, 8, MESSAGE), jnp.bfloat16),
            jax.ShapeDtypeStruct((64,), jnp.float32),
        ],
        in_specs=[pl.BlockSpec(memory_space=pltpu.HBM)] * 4 + smem(5),
        out_specs=vmem(1) + smem(1),
        scratch_shapes=[
            pltpu.VMEM((CAP, 2, TILES * LANES), jnp.bfloat16),
            pltpu.VMEM((TILES, LANES), jnp.int32),
            pltpu.VMEM((TILES, LANES), jnp.float32),
            pltpu.VMEM((TILES, LANES), jnp.float32),
            pltpu.VMEM((2, 8, TILES * LANES), jnp.float32),
            pltpu.VMEM((2, TILES, LANES), jnp.float32),
            pltpu.SemaphoreType.DMA((4,)),
        ],
        compiler_params=pltpu.CompilerParams(vmem_limit_bytes=66500000),
        name="pack",
    )(
        packed,
        trap_index.reshape(TILES, LANES),
        mean_field.reshape(TILES, LANES),
        pairing.reshape(TILES, LANES),
        trap_table,
        counts,
        slot_slice,
        occupation,
        filter_coef,
    )
    message = lax.all_to_all(message, "slab", 0, 0, tiled=True)
    low = lax.ppermute(message[:, :, MESSAGE - HALO :], "slab", neighbours(1))
    high = lax.ppermute(message[:, :, :HALO], "slab", neighbours(-1))
    parts = filter_call(low, message, high, terms)
    parts = lax.all_to_all(
        parts, ("cuts", "slab"), 0, 0, axis_index_groups=summing_groups(), tiled=True
    )
    sums = pl.pallas_call(
        sum_kernel,
        out_shape=jax.ShapeDtypeStruct((1, 2 * 288), jnp.float32),
        in_specs=vmem(1),
        out_specs=pl.BlockSpec(memory_space=pltpu.VMEM),
        compiler_params=grant(4),
        name="total",
    )(parts)
    sums = lax.ppermute(sums, ("cuts", "slab"), routes())
    offset = lax.axis_index("cuts") * share
    mean_local = lax.dynamic_slice_in_dim(mean_field, offset, share, 1)
    pairing_local = lax.dynamic_slice_in_dim(pairing, offset, share, 1)
    normal_density = sums[:, :share]
    anomalous_density = sums[:, share:]
    cube_root = jnp.cbrt(normal_density + density_floor)
    new_mean_field = 0.5 * mean_local + 0.5 * (beta_coef * cube_root * cube_root - chem_level)
    new_pairing = 0.5 * pairing_local - coupling * anomalous_density
    return (normal_density, anomalous_density, new_mean_field, new_pairing)


def solution(mesh):
    return jax.shard_map(
        body,
        mesh=mesh,
        in_specs=(
            P(None, "cuts", "slab", None),
            P(),
            P(),
            P(),
            P(),
            P("slab", None),
            P(),
            P("slab", None),
            P("slab", None),
        ),
        out_specs=(P("slab", "cuts"), P("slab", "cuts"), P("slab", "cuts"), P("slab", "cuts")),
        check_vma=False,
    )
```
